32 devices in a mesh: samp: 4 (over z), atom: 8 (over y, x, core).
Axes of the slice: x: 2, y: 2, z: 4, core: 2. Of those that a mesh axis runs over, the one named last changes fastest.
Arguments:
- atom_state: bfloat16 [16, 2560, 128], P('samp', 'atom'), may hold values from -6 to 6, as said below
- atom_token: int32 [2560], P('atom'), may hold values from 0 to 319, never falling along the last dimension, each value on 1 to 24 neighbouring positions
- window_valid: int32 [80], P('atom'), may hold values from 1 to 32
- attend_gain: float32 [128], replicated, may hold values from 0.25 to 1.75
- project_weight: bfloat16 [128, 384], replicated, may hold values from -4 to 4
- output_weight: bfloat16 [128, 128], replicated, may hold values from -1.5 to 1.5
- token_bias: float32 [4], replicated, may hold values from -2 to 2
- transit_gain: float32 [128], replicated, may hold values from 0.25 to 1.75
- transit_weight: bfloat16 [128, 512], replicated, may hold values from -0.5 to 0.5
- return_weight: bfloat16 [256, 128], replicated, may hold values from -0.375 to 0.375
- cotangent: bfloat16 [16, 2560, 128], P('samp', 'atom'), may hold values from -6 to 6
Outputs:
- block_out: bfloat16 [16, 2560, 128], P('samp', 'atom')
- state_grad: bfloat16 [16, 2560, 128], P('samp', 'atom')
- grad_attend_gain: float32 [128], replicated
- grad_project: float32 [128, 384], replicated
- grad_output: float32 [128, 128], replicated
- grad_bias: float32 [4], replicated
- grad_transit_gain: float32 [128], replicated
- grad_transit: float32 [128, 512], replicated
- grad_return: float32 [256, 128], replicated
The draws below stay inside these ranges and needn't reach their ends.
Inputs may be any that keep to these rules, and one draw needn't show every extreme that they name: atom_state is finite. `atom_token`: tokens are numbered in order along the atoms; a token has 1 to 24 atoms.
All inputs are finite; a program needn't handle non-finite values.
Results may differ from the reference program's by a relative error of at most 0.025.
The reference program's roundings to bfloat16 on the way (of `normed`, `projected`, `attended`, `residual`, `transit_in`, `gated`, `back_hidden` and `back_res16`) count: a program that leaves them out, or rounds other values in their place, can miss the bound.
Values may be sent and summed in bfloat16 or wider, within the bound.
No kernel may reach another device: no remote copies, remote signals or barrier semaphores. Data moves between devices by JAX's collectives and lax.ppermute only.
A program may use at most 64 MiB of HBM per device.

```python
import math
import jax
import jax.numpy as jnp
import numpy as np
from jax import lax

WIDTH = 128
HEADS = 4
TRANS = 256
QWIN = 32
KWIN = 128
HALO = 48
SAMPLES = 16
ATOMS = 2560
WINDOWS = 80
TOKENS = 320


def draw_atom_state(key, part):
    extent = (SAMPLES, ATOMS, WIDTH)
    values = jnp.clip(jax.random.normal(jax.random.fold_in(key, 15), extent, jnp.float32), -6.0, 6.0)
    return values.astype(jnp.bfloat16)


def draw_project_weight(key, part):
    base = jnp.clip(jax.random.normal(jax.random.fold_in(key, 21), (WIDTH, 3 * WIDTH), jnp.float32), -6.0, 6.0)
    base = base / jnp.sqrt(float(WIDTH))
    return base.astype(jnp.bfloat16)


def with_ends(array, own_key, low, high):
    place = [jax.random.randint(jax.random.fold_in(own_key, axis), (), 0, length) for axis, length in enumerate(array.shape)]
    main_axis = array.shape.index(max(array.shape))
    next_to = place[:main_axis] + [(place[main_axis] + 1) % array.shape[main_axis]] + place[main_axis + 1:]
    return array.at[tuple(place)].set(low).at[tuple(next_to)].set(high)


def steps_of(key, dims, split, smallest, largest):
    factor_of, own = 1.0, jax.random.fold_in(key, 6)
    for dim, parts in split:
        heights = jnp.exp(jax.random.uniform(jax.random.fold_in(own, dim), (parts,), jnp.float32, smallest / len(split), largest / len(split)))
        factor_of = factor_of * jnp.repeat(heights, dims[dim] // parts).reshape([-1 if axis == dim else 1 for axis in range(len(dims))])
    return factor_of


def split_up(number_of, total, reach, slope):
    loads = [(1 << 20) // math.isqrt(rank ** slope) + 1 for rank in range(2, number_of + 1)]
    spare, holding = total - reach - (number_of - 1), [1] * (number_of - 1)
    while spare > 0:
        candidates = [i for i in range(number_of - 1) if holding[i] < reach]
        mass, remaining = sum([loads[i] for i in candidates]), spare
        for i in candidates:
            more = min(reach - holding[i], max(1, remaining * loads[i] // mass), spare)
            holding[i] = holding[i] + more
            spare = spare - more
    return np.array([reach] + holding)


def ragged_sizes(own_key, count, total, limit, skew):
    if count == 2:
        one = jax.random.randint(own_key, (), max(1, total - limit), min(limit, total - 1) + 1)
        return jnp.stack([one, total - one])
    tallies = jnp.asarray(split_up(count, total, limit, skew), jnp.int32)
    twos = (count - 1) // 2
    donor, sink = tallies[1:1 + 2 * twos:2], tallies[2:2 + 2 * twos:2]
    margin = jnp.minimum(donor - 1, limit - sink)
    moved = jax.random.randint(jax.random.fold_in(own_key, 1), (twos,), 0, 1 << 20) % (margin + 1)
    tallies = tallies.at[1:1 + 2 * twos:2].set(donor - moved).at[2:2 + 2 * twos:2].set(sink + moved)
    return tallies[jax.random.permutation(jax.random.fold_in(own_key, 2), count)]


def bell_draw(stream_key, shape, scale, most, cuts=(), dtype=jnp.bfloat16):
    values = jax.random.normal(stream_key, shape, jnp.float32) * scale
    if len(cuts) > 0:
        values = steps_of(stream_key, shape, cuts, -0.22, 0.18) * values
    return jnp.clip(values, min=-most, max=most).astype(dtype)


def setup_inputs(seed: int = 0) -> dict:
    arg_keys = jax.random.split(jax.random.key(seed), 12)
    atom_state = draw_atom_state(jax.random.fold_in(arg_keys[11], 71), 0)
    atom_token = jnp.searchsorted(jnp.cumsum(ragged_sizes(arg_keys[1], TOKENS, ATOMS, 24, 0)), jnp.arange(ATOMS), side="right").astype(jnp.int32)
    window_valid = with_ends(jax.random.randint(arg_keys[2], (WINDOWS,), 1, QWIN + 1), jax.random.fold_in(arg_keys[2], 1), 1, QWIN).astype(jnp.int32)
    attend_gain = jnp.clip(1.0 + 0.15 * jax.random.normal(arg_keys[3], (WIDTH,), jnp.float32), 0.25, 1.75)
    project_weight = draw_project_weight(jax.random.fold_in(arg_keys[11], 71), 0)
    output_weight = bell_draw(arg_keys[5], (WIDTH, WIDTH), (WIDTH // 8) ** -0.5, 1.5)
    token_bias = jnp.clip(jax.random.uniform(arg_keys[6], (HEADS,), jnp.float32, -2.0, 2.0), -2.0, 2.0)
    transit_gain = jnp.clip(1.0 + 0.15 * jax.random.normal(arg_keys[7], (WIDTH,), jnp.float32), 0.25, 1.75)
    transit_weight = bell_draw(arg_keys[8], (WIDTH, 2 * TRANS), WIDTH ** -0.5, 0.5)
    return_weight = bell_draw(arg_keys[9], (TRANS, WIDTH), TRANS ** -0.5, 0.375)
    cotangent = bell_draw(arg_keys[10], (SAMPLES, ATOMS, WIDTH), 1.0, 6.0, ((0, 4), (1, 8)))
    return {"atom_state": atom_state, "atom_token": atom_token, "window_valid": window_valid, "attend_gain": attend_gain, "project_weight": project_weight, "output_weight": output_weight, "token_bias": token_bias, "transit_gain": transit_gain, "transit_weight": transit_weight, "return_weight": return_weight, "cotangent": cotangent}


PRECISE = lax.Precision.HIGHEST
EPSILON = 1e-05
CLIP_NORM = 256.0

def normalize(values, scaling):
    values = values.astype(jnp.float32)
    center = lax.optimization_barrier(jnp.mean(values, axis=-1, keepdims=True))
    shifted = values - center
    variance = lax.optimization_barrier(jnp.mean(shifted * shifted, axis=-1, keepdims=True))
    return shifted * lax.rsqrt(variance + EPSILON) * scaling

def token_codes(atom_token, window_valid):
    windows_here = window_valid.shape[0]
    slots = lax.broadcasted_iota(jnp.int32, (windows_here, QWIN), 1)
    inside = (slots < window_valid[:, None]).reshape(-1)
    return jnp.where(inside, atom_token + 1, 0).astype(jnp.int32)

def attend(queries, pairs, query_ids, ext_ids, token_bias):
    channels = queries.shape[1]
    window_count = queries.shape[0] // QWIN
    extra_blocks = 2 * HALO // QWIN
    span_blocks = KWIN // QWIN
    head_dim = channels // HEADS
    blocks = pairs.reshape(window_count + extra_blocks, QWIN, 2 * channels)
    gathered = jnp.concatenate([blocks[offset:offset + window_count] for offset in range(span_blocks)], axis=1)
    code_blocks = ext_ids.reshape(window_count + extra_blocks, QWIN)
    key_ids = jnp.concatenate([code_blocks[offset:offset + window_count] for offset in range(span_blocks)], axis=1)
    query_blocks = queries.reshape(window_count, QWIN, HEADS, head_dim)
    keys_in = gathered[:, :, :channels].reshape(window_count, KWIN, HEADS, head_dim)
    values_in = gathered[:, :, channels:].reshape(window_count, KWIN, HEADS, head_dim)
    scores = jnp.einsum('wqhd,wkhd->whqk', query_blocks, keys_in, precision=PRECISE) / jnp.sqrt(float(head_dim))
    query_codes = query_ids.reshape(window_count, QWIN)
    same_token = (query_codes[:, :, None] == key_ids[:, None, :]).astype(jnp.float32)
    scores = scores + token_bias[None, :, None, None] * same_token[:, None, :, :]
    usable_key = (key_ids > 0)[:, None, None, :]
    scores = jnp.where(usable_key, scores, -1e+30)
    highest = lax.stop_gradient(lax.optimization_barrier(jnp.max(scores, axis=-1, keepdims=True)))
    weights = jnp.exp(scores - highest)
    weights = weights / lax.optimization_barrier(jnp.sum(weights, axis=-1, keepdims=True))
    outcome = jnp.einsum('whqk,wkhd->wqhd', weights, values_in, precision=PRECISE)
    return outcome.reshape(window_count * QWIN, channels)

def reference(atom_state, atom_token, window_valid, attend_gain, project_weight, output_weight, token_bias, transit_gain, transit_weight, return_weight, cotangent):
    query_ids = token_codes(atom_token, window_valid)
    ext_ids = jnp.pad(query_ids, (HALO, HALO))
    channels = atom_state.shape[2]
    atom_total = atom_state.shape[1]

    def one_sample(carry, operands):
        state_rows, cot_rows = operands
        normed = normalize(state_rows, attend_gain).astype(jnp.bfloat16)
        projected = jnp.dot(normed, project_weight, preferred_element_type=jnp.float32).astype(jnp.bfloat16)
        queries = projected[:, :channels]
        pairs = jnp.pad(projected[:, channels:], ((HALO, HALO), (0, 0)))

        def local_attend(query_in, pairs_in, bias_in):
            return attend(query_in, pairs_in, query_ids, ext_ids, bias_in)
        outcome, pull_attend = jax.vjp(local_attend, queries.astype(jnp.float32), pairs.astype(jnp.float32), token_bias)
        attended = outcome.astype(jnp.bfloat16)
        residual = (state_rows.astype(jnp.float32) + jnp.dot(attended, output_weight, preferred_element_type=jnp.float32)).astype(jnp.bfloat16)
        transit_in = normalize(residual, transit_gain).astype(jnp.bfloat16)
        both_parts = jnp.dot(transit_in, transit_weight, preferred_element_type=jnp.float32)
        gate_part = both_parts[:, :TRANS]
        up_part = both_parts[:, TRANS:]
        gated = (jax.nn.silu(gate_part) * up_part).astype(jnp.bfloat16)
        block_rows = (residual.astype(jnp.float32) + jnp.dot(gated, return_weight, preferred_element_type=jnp.float32)).astype(jnp.bfloat16)
        grad_return = jnp.dot(gated.T, cot_rows, preferred_element_type=jnp.float32)
        back_gated = jnp.dot(cot_rows, return_weight.T, preferred_element_type=jnp.float32)
        sigmoid_gate = jax.nn.sigmoid(gate_part)
        back_gate = back_gated * up_part * sigmoid_gate * (1.0 + gate_part * (1.0 - sigmoid_gate))
        back_up = back_gated * gate_part * sigmoid_gate
        back_hidden = jnp.concatenate([back_gate, back_up], axis=1).astype(jnp.bfloat16)
        grad_transit = jnp.dot(transit_in.T, back_hidden, preferred_element_type=jnp.float32)
        back_transit = jnp.dot(back_hidden, transit_weight.T, preferred_element_type=jnp.float32)
        _, pull_second = jax.vjp(normalize, residual.astype(jnp.float32), transit_gain)
        back_res_norm, grad_transit_gain = pull_second(back_transit)
        back_residual = cot_rows.astype(jnp.float32) + back_res_norm
        back_res16 = back_residual.astype(jnp.bfloat16)
        grad_output = jnp.dot(attended.T, back_res16, preferred_element_type=jnp.float32)
        back_attended = jnp.dot(back_res16, output_weight.T, preferred_element_type=jnp.float32)
        back_queries, back_pairs, grad_bias = pull_attend(back_attended)
        back_projected = jnp.concatenate([back_queries, back_pairs[HALO:HALO + atom_total]], axis=1)
        grad_project = jnp.dot(normed.astype(jnp.float32).T, back_projected, precision=PRECISE)
        back_normed = jnp.dot(back_projected, project_weight.astype(jnp.float32).T, precision=PRECISE)
        _, pull_first = jax.vjp(normalize, state_rows.astype(jnp.float32), attend_gain)
        back_state_norm, grad_attend_gain = pull_first(back_normed)
        state_rows_grad = (back_residual + back_state_norm).astype(jnp.bfloat16)
        terms = (grad_attend_gain, grad_project, grad_output, grad_bias, grad_transit_gain, grad_transit, grad_return)
        carry = tuple((total + member for total, member in zip(carry, terms)))
        return (carry, (block_rows, state_rows_grad))
    start = (jnp.zeros((channels,), jnp.float32), jnp.zeros((channels, 3 * channels), jnp.float32), jnp.zeros((channels, channels), jnp.float32), jnp.zeros((HEADS,), jnp.float32), jnp.zeros((channels,), jnp.float32), jnp.zeros((channels, 2 * TRANS), jnp.float32), jnp.zeros((TRANS, channels), jnp.float32))
    totals, (block_out, state_grad) = lax.scan(one_sample, start, (atom_state, cotangent))
    squares = sum((jnp.sum(member * member) for member in totals))
    factor = CLIP_NORM / jnp.sqrt(squares + CLIP_NORM * CLIP_NORM)
    clipped = tuple((member * factor for member in totals))
    return (block_out, state_grad, clipped[0], clipped[1], clipped[2], clipped[3], clipped[4], clipped[5], clipped[6])
```

```python
import functools
import math

import jax
import jax.numpy as jnp
from jax import lax
from jax.experimental import pallas as pl
from jax.experimental.pallas import tpu as pltpu
from jax.sharding import PartitionSpec as P

HEADS = 4
TRANS = 256
QWIN = 32
KWIN = 128
HALO = 48
EPSILON = 1e-05
CLIP_NORM = 256.0
LANES = 128
SMALL_ROWS = 64
LOG2E = 1.0 / math.log(2.0)

F32 = jnp.float32
BF16 = jnp.bfloat16


def mm(a, b):
    return lax.dot_general(a, b, (((1,), (0,)), ((), ())), preferred_element_type=F32)


def mm_nt(a, b):
    return lax.dot_general(a, b, (((1,), (1,)), ((), ())), preferred_element_type=F32)


def mm_tn(a, b):
    return lax.dot_general(a, b, (((0,), (0,)), ((), ())), preferred_element_type=F32)


def row_mean(x):
    return jnp.sum(x, axis=-1, keepdims=True) * (1.0 / x.shape[-1])


def column_sum(x):
    return jnp.sum(x, axis=0, keepdims=True)


def split_norm(x):
    shifted = x - row_mean(x)
    inverse = lax.rsqrt(row_mean(shifted * shifted) + EPSILON)
    return shifted * inverse, inverse


def norm_grad(grad, unit, inverse):
    return inverse * (grad - row_mean(grad) - unit * row_mean(grad * unit))


def head_of_lane(rows):
    return lax.broadcasted_iota(jnp.int32, (rows, LANES), 1) // (LANES // HEADS)


def spread_heads(rows):
    head = head_of_lane(QWIN)
    return jnp.concatenate(
        [jnp.where(head == h, rows, jnp.zeros_like(rows)) for h in range(HEADS)], axis=0
    )


def gather_heads(rows):
    head = head_of_lane(QWIN)
    total = rows[:QWIN]
    for h in range(1, HEADS):
        total = jnp.where(head == h, rows[h * QWIN : (h + 1) * QWIN], total)
    return total


def block_kernel(
    flags,
    state,
    pair_rows,
    link_rows,
    own_codes,
    attend_gain,
    project_weight,
    output_weight,
    bias_row,
    transit_gain,
    transit_weight,
    return_weight,
    cot,
    block_out,
    back_norm,
    back_res,
    to_before,
    to_after,
    keep,
    send,
    norm_ext,
    unit_ext,
    q_all,
    k_all,
    v_all,
    codes,
    probs,
    att,
    d_att,
    dq_all,
    dk_all,
    dv_all,
    grads,
    bias_acc,
):
    samples, atoms, channels = state.shape
    ext = atoms + 2 * HALO
    windows = atoms // QWIN
    is_odd = flags[0] == 1
    halo_rows = samples * HALO
    scale = 1.0 / math.sqrt(channels // HEADS)

    before = jnp.where(is_odd, pair_rows[...], link_rows[...])
    after = jnp.where(is_odd, link_rows[...], pair_rows[...])

    def edge_codes(part):
        high = part[halo_rows : halo_rows + 1, :].astype(F32)
        low = part[halo_rows + 1 : halo_rows + 2, :].astype(F32)
        return high * 256.0 + low

    def down_lanes(row):
        return jnp.transpose(jnp.broadcast_to(row, (LANES, LANES)))

    codes[0:HALO, :] = down_lanes(edge_codes(before))[0:HALO]
    for i in range(own_codes.shape[0]):
        count = min(LANES, atoms - i * LANES)
        codes[HALO + i * LANES : HALO + i * LANES + count, :] = down_lanes(own_codes[i : i + 1, :])[0:count]
    codes[HALO + atoms : ext, :] = down_lanes(edge_codes(after))[0:HALO]

    grads[...] = jnp.zeros_like(grads)
    bias_acc[...] = jnp.zeros_like(bias_acc)
    dk_all[...] = jnp.zeros_like(dk_all)
    dv_all[...] = jnp.zeros_like(dv_all)

    gain_one = attend_gain[...]
    gain_two = transit_gain[...]
    for s in range(samples):
        rows = jnp.concatenate(
            [before[s * HALO : (s + 1) * HALO], state[s], after[s * HALO : (s + 1) * HALO]], axis=0
        ).astype(F32)
        unit, _ = split_norm(rows)
        unit_ext[s] = unit
        normed = (unit * gain_one).astype(BF16)
        norm_ext[s] = normed
        projected = mm(normed, project_weight[...]).astype(BF16)
        q_all[s] = projected[HALO : HALO + atoms, :channels]
        k_all[s] = projected[:, channels : 2 * channels]
        v_all[s] = projected[:, 2 * channels :]

    def window_mask(start):
        key_code = codes[pl.ds(start, KWIN), :]
        query = codes[pl.ds(start + HALO, QWIN), :]
        query_code = jnp.transpose(jnp.concatenate([query] * HEADS, axis=0))
        return key_code, key_code == query_code

    def forward_window(w, carry):
        start = pl.multiple_of(w * QWIN, QWIN)
        key_code, same = window_mask(start)
        offset = jnp.where(same, bias_row[...] * LOG2E, 0.0)
        offset = jnp.where(key_code > 0, offset, -1e30)
        for s in range(samples):
            queries = spread_heads(q_all[s, pl.ds(start, QWIN), :])
            keys = k_all[s, pl.ds(start, KWIN), :]
            values = v_all[s, pl.ds(start, KWIN), :]
            scores = mm_nt(keys, queries) * (scale * LOG2E) + offset
            weights = jnp.exp2(scores - jnp.max(scores, axis=0, keepdims=True))
            weights = weights * (1.0 / column_sum(weights))
            probs[w * samples + s] = weights
            outcome = gather_heads(mm_tn(weights.astype(BF16), values))
            att[s, pl.ds(start, QWIN), :] = outcome.astype(BF16)
        return carry

    lax.fori_loop(0, windows, forward_window, 0)

    def transition(s, gain_grad):
        attended = att[s]
        residual = (state[s].astype(F32) + mm(attended, output_weight[...])).astype(BF16)
        residual = residual.astype(F32)
        unit, inverse = split_norm(residual)
        transit_in = (unit * gain_two).astype(BF16)
        both = mm(transit_in, transit_weight[...])
        gate = both[:, :TRANS]
        up = both[:, TRANS:]
        sigmoid = 1.0 / (1.0 + jnp.exp(-gate))
        silu = gate * sigmoid
        gated = (silu * up).astype(BF16)
        block_out[s] = (residual + mm(gated, return_weight[...])).astype(BF16)
        cot16 = cot[s]
        back_gated = mm_nt(cot16, return_weight[...])
        back_gate = back_gated * up * sigmoid * (1.0 + gate * (1.0 - sigmoid))
        back_hidden = jnp.concatenate([back_gate, back_gated * silu], axis=1).astype(BF16)
        grads[pl.ds(8 * channels, TRANS), :] += mm_tn(gated, cot16)
        grad_transit = mm_tn(transit_in, back_hidden)
        for i in range(2 * TRANS // LANES):
            grads[pl.ds((4 + i) * channels, channels), :] += grad_transit[:, i * LANES : (i + 1) * LANES]
        back_transit = mm_nt(back_hidden, transit_weight[...])
        gain_grad = gain_grad + column_sum(back_transit * unit)
        back_residual = cot16.astype(F32) + norm_grad(back_transit * gain_two, unit, inverse)
        back_res[s] = back_residual
        back16 = back_residual.astype(BF16)
        grads[pl.ds(3 * channels, channels), :] += mm_tn(attended, back16)
        d_att[s] = mm_nt(back16, output_weight[...]).astype(BF16)
        return gain_grad

    zero_row = jnp.zeros((1, channels), F32)
    gain_grad_two = lax.fori_loop(0, samples, transition, zero_row)

    def backward_window(w, carry):
        start = pl.multiple_of(w * QWIN, QWIN)
        _, same = window_mask(start)
        bias_part = None
        for s in range(samples):
            queries = spread_heads(q_all[s, pl.ds(start, QWIN), :])
            back = spread_heads(d_att[s, pl.ds(start, QWIN), :])
            keys = k_all[s, pl.ds(start, KWIN), :]
            values = v_all[s, pl.ds(start, KWIN), :]
            weights = probs[w * samples + s]
            back_weights = mm_nt(values, back)
            weighted = weights * back_weights
            back_scores = weighted - weights * column_sum(weighted)
            bias_part = back_scores if bias_part is None else bias_part + back_scores
            scores16 = back_scores.astype(BF16)
            span = pl.ds(start, KWIN)
            dv_all[s, span, :] += mm(weights.astype(BF16), back)
            dk_all[s, span, :] += mm(scores16, queries)
            dq_all[s, pl.ds(start, QWIN), :] = gather_heads(mm_tn(scores16, keys))
        bias_acc[...] += jnp.where(same, bias_part, 0.0)
        return carry

    lax.fori_loop(0, windows, backward_window, 0)

    rim = jnp.zeros((HALO, channels), BF16)

    def projection(s, gain_grad):
        back_q = (dq_all[s] * scale).astype(BF16)
        back_q = jnp.concatenate([rim, back_q, rim], axis=0)
        back_k = (dk_all[s] * scale).astype(BF16)
        back_v = dv_all[s].astype(BF16)
        back_all = jnp.concatenate([back_q, back_k, back_v], axis=1)
        back_normed = mm_nt(back_all, project_weight[...])
        grad_project = mm_tn(norm_ext[s], back_all)
        for i in range(3):
            grads[pl.ds(i * channels, channels), :] += grad_project[:, i * LANES : (i + 1) * LANES]
        gain_grad = gain_grad + column_sum(back_normed * unit_ext[s])
        back_norm[s] = back_normed[HALO : HALO + atoms]
        rows = pl.ds(pl.multiple_of(s * HALO, HALO), HALO)
        to_before[rows, :] = back_normed[:HALO].astype(BF16)
        to_after[rows, :] = back_normed[HALO + atoms :].astype(BF16)
        return gain_grad

    gain_grad_one = lax.fori_loop(0, samples, projection, zero_row)

    tail = 8 * channels + TRANS
    grads[pl.ds(tail, 1), :] = gain_grad_one
    grads[pl.ds(tail + 1, 1), :] = gain_grad_two
    grads[pl.ds(tail + 2, 1), :] = column_sum(bias_acc[...])

    half = keep.shape[0]
    mine = flags[1]
    keep[...] = grads[pl.ds(pl.multiple_of(mine * half, 8), half), :].astype(BF16)
    send[...] = grads[pl.ds(pl.multiple_of((1 - mine) * half, 8), half), :].astype(BF16)


def rim_kernel(flags, state, gain, back_norm, back_res, pair_back, link_back, out):
    samples, atoms, channels = state.shape
    is_odd = flags[0] == 1
    from_before = jnp.where(is_odd, pair_back[...], link_back[...]).astype(F32)
    from_after = jnp.where(is_odd, link_back[...], pair_back[...]).astype(F32)
    for s in range(samples):
        grad = back_norm[s]
        part = slice(s * HALO, (s + 1) * HALO)
        grad = jnp.concatenate(
            [
                grad[:HALO] + from_before[part],
                grad[HALO : atoms - HALO],
                grad[atoms - HALO :] + from_after[part],
            ],
            axis=0,
        )
        unit, inverse = split_norm(state[s].astype(F32))
        out[s] = (back_res[s] + norm_grad(grad * gain[...], unit, inverse)).astype(BF16)


def clip_kernel(flags, own, other, attend, project, output, bias, transit_gain, transit, back):
    first = flags[0] == 0
    channels = LANES
    low = jnp.where(first, own[...], other[...]).astype(F32)
    high = jnp.where(first, other[...], own[...]).astype(F32)
    total = jnp.concatenate([low, high], axis=0)
    tail = 8 * channels + TRANS
    lane = lax.broadcasted_iota(jnp.int32, (1, LANES), 1)
    bias_row = total[tail + 2 : tail + 3]
    width = LANES // HEADS
    heads = jnp.zeros((1, LANES), F32)
    for h in range(HEADS):
        inside = (lane >= h * width) & (lane < (h + 1) * width)
        sum_h = jnp.sum(jnp.where(inside, bias_row, 0.0), axis=1, keepdims=True)
        heads = jnp.where(lane == h, sum_h, heads)
    plain = total[: tail + 2]
    squares = jnp.sum(column_sum(plain * plain) + heads * heads, axis=1, keepdims=True)
    factor = CLIP_NORM * lax.rsqrt(squares + CLIP_NORM * CLIP_NORM)
    for i in range(3):
        project[:, i * LANES : (i + 1) * LANES] = total[i * channels : (i + 1) * channels] * factor
    output[...] = total[3 * channels : 4 * channels] * factor
    for i in range(2 * TRANS // LANES):
        transit[:, i * LANES : (i + 1) * LANES] = total[(4 + i) * channels : (5 + i) * channels] * factor
    back[...] = total[8 * channels : 8 * channels + TRANS] * factor
    attend[...] = total[tail : tail + 1] * factor
    transit_gain[...] = total[tail + 1 : tail + 2] * factor
    bias[...] = heads * factor


def swap(value, axis, mask):
    return lax.ppermute(value, axis, [(i, i ^ mask) for i in range(lax.axis_size(axis))])


def pair_exchange(to_partner, to_link, axis):
    size = lax.axis_size(axis)
    links = [(i, i + 1) for i in range(1, size - 1, 2)]
    links = links + [(j, i) for i, j in links]
    return lax.ppermute(to_link, axis, links), swap(to_partner, axis, 1)


def token_codes(atom_token, window_valid):
    windows_here = window_valid.shape[0]
    slots = lax.broadcasted_iota(jnp.int32, (windows_here, QWIN), 1)
    inside = (slots < window_valid[:, None]).reshape(-1)
    return jnp.where(inside, atom_token + 1, 0)


def edge_pack(state, codes, at_end):
    samples, atoms, channels = state.shape
    start = jnp.where(at_end, atoms - HALO, 0)
    rows = lax.dynamic_slice_in_dim(state, start, HALO, axis=1).reshape(samples * HALO, channels)
    part = lax.dynamic_slice_in_dim(codes, start, HALO, axis=0)
    digits = jnp.stack([part // 256, part % 256]).astype(BF16)
    digits = jnp.pad(digits, ((0, 14), (0, channels - HALO)))
    return jnp.concatenate([rows, digits], axis=0)


def whole(*shape):
    return pl.BlockSpec(memory_space=pltpu.VMEM)


def call(kernel, operands, outs, scratch=(), flops=0):
    vmem = pl.BlockSpec(memory_space=pltpu.VMEM)
    smem = pl.BlockSpec(memory_space=pltpu.SMEM)
    moved = sum(x.size * x.dtype.itemsize for x in operands)
    return pl.pallas_call(
        kernel,
        out_shape=[jax.ShapeDtypeStruct(shape, dtype) for shape, dtype in outs],
        in_specs=[smem] + [vmem] * (len(operands) - 1),
        out_specs=[vmem] * len(outs),
        scratch_shapes=list(scratch),
        cost_estimate=pl.CostEstimate(flops=flops, bytes_accessed=moved, transcendentals=0),
        compiler_params=pltpu.CompilerParams(vmem_limit_bytes=48 * 1024 * 1024),
    )(*operands)


def on_device(
    atom_state,
    atom_token,
    window_valid,
    attend_gain,
    project_weight,
    output_weight,
    token_bias,
    transit_gain,
    transit_weight,
    return_weight,
    cotangent,
):
    samples, atoms, channels = atom_state.shape
    ext = atoms + 2 * HALO
    windows = atoms // QWIN
    place = lax.axis_index("atom")
    odd = place % 2
    codes = token_codes(atom_token, window_valid)
    link_rows, pair_rows = pair_exchange(
        edge_pack(atom_state, codes, odd == 0), edge_pack(atom_state, codes, odd == 1), "atom"
    )
    code_rows = -(-atoms // LANES)
    own_codes = jnp.pad(codes.astype(F32), (0, code_rows * LANES - atoms)).reshape(code_rows, LANES)
    flags = jnp.stack([odd, odd]).astype(jnp.int32)
    total_rows = 8 * channels + TRANS + SMALL_ROWS
    half = total_rows // 2
    halo_rows = samples * HALO
    block_out, back_norm, back_res, to_before, to_after, keep, send = call(
        block_kernel,
        (
            flags,
            atom_state,
            pair_rows,
            link_rows,
            own_codes,
            attend_gain.reshape(1, channels),
            project_weight,
            output_weight,
            jnp.repeat(token_bias, QWIN).reshape(1, HEADS * QWIN),
            transit_gain.reshape(1, channels),
            transit_weight,
            return_weight,
            cotangent,
        ),
        (
            ((samples, atoms, channels), BF16),
            ((samples, atoms, channels), F32),
            ((samples, atoms, channels), F32),
            ((halo_rows, channels), BF16),
            ((halo_rows, channels), BF16),
            ((half, channels), BF16),
            ((half, channels), BF16),
        ),
        (
            pltpu.VMEM((samples, ext, channels), BF16),
            pltpu.VMEM((samples, ext, channels), F32),
            pltpu.VMEM((samples, atoms, channels), BF16),
            pltpu.VMEM((samples, ext, channels), BF16),
            pltpu.VMEM((samples, ext, channels), BF16),
            pltpu.VMEM((ext, LANES), F32),
            pltpu.VMEM((windows * samples, KWIN, HEADS * QWIN), F32),
            pltpu.VMEM((samples, atoms, channels), BF16),
            pltpu.VMEM((samples, atoms, channels), BF16),
            pltpu.VMEM((samples, atoms, channels), F32),
            pltpu.VMEM((samples, ext, channels), F32),
            pltpu.VMEM((samples, ext, channels), F32),
            pltpu.VMEM((total_rows, channels), F32),
            pltpu.VMEM((KWIN, HEADS * QWIN), F32),
        ),
        flops=4_000_000_000,
    )

    got = swap(send, "atom", 1)
    part = keep + got
    x_bit = (place // 2) % 2
    quarter = half // 2
    mine = lax.dynamic_slice_in_dim(part, x_bit * quarter, quarter)
    theirs = lax.dynamic_slice_in_dim(part, (1 - x_bit) * quarter, quarter)
    sums = mine + swap(theirs, "atom", 2)
    mask = 4
    while mask < lax.axis_size("atom"):
        sums = sums + swap(sums, "atom", mask)
        mask *= 2
    mask = 1
    while mask < lax.axis_size("samp"):
        sums = sums + swap(sums, "samp", mask)
        mask *= 2
    other = swap(sums, "atom", 2)
    sums = jnp.where(
        x_bit == 0,
        jnp.concatenate([sums, other], axis=0),
        jnp.concatenate([other, sums], axis=0),
    )
    other = swap(sums, "atom", 1)
    clipped = call(
        clip_kernel,
        (flags, sums, other),
        (
            ((1, channels), F32),
            ((channels, 3 * channels), F32),
            ((channels, channels), F32),
            ((1, LANES), F32),
            ((1, channels), F32),
            ((channels, 2 * TRANS), F32),
            ((TRANS, channels), F32),
        ),
    )

    odd_here = odd == 1
    to_link = jnp.where(odd_here, to_after, to_before)
    to_partner = jnp.where(odd_here, to_before, to_after)
    link_back, pair_back = pair_exchange(to_partner, to_link, "atom")
    (state_grad,) = call(
        rim_kernel,
        (flags, atom_state, attend_gain.reshape(1, channels), back_norm, back_res, pair_back, link_back),
        (((samples, atoms, channels), BF16),),
        flops=100_000_000,
    )
    return (
        block_out,
        state_grad,
        clipped[0].reshape(channels),
        clipped[1],
        clipped[2],
        clipped[3][0, :HEADS],
        clipped[4].reshape(channels),
        clipped[5],
        clipped[6],
    )


def solution(mesh):
    return jax.shard_map(
        on_device,
        mesh=mesh,
        in_specs=(
            P("samp", "atom", None),
            P("atom"),
            P("atom"),
            P(),
            P(),
            P(),
            P(),
            P(),
            P(),
            P(),
            P("samp", "atom", None),
        ),
        out_specs=(
            P("samp", "atom", None),
            P("samp", "atom", None),
            P(),
            P(),
            P(),
            P(),
            P(),
            P(),
            P(),
        ),
        check_vma=False,
    )
```

```python
import functools
import math

import jax
import jax.numpy as jnp
from jax import lax
from jax.experimental import pallas as pl
from jax.experimental.pallas import tpu as pltpu
from jax.sharding import PartitionSpec as P

HEADS = 4
TRANS = 256
QWIN = 32
KWIN = 128
HALO = 48
EPSILON = 1e-05
CLIP_NORM = 256.0
LANES = 128
GROUP = 2
SLOT = 16
LOG2E = 1.0 / math.log(2.0)

F32 = jnp.float32
BF16 = jnp.bfloat16


def mm(a, b):
    return lax.dot_general(a, b, (((1,), (0,)), ((), ())), preferred_element_type=F32)


def mm_nt(a, b):
    return lax.dot_general(a, b, (((1,), (1,)), ((), ())), preferred_element_type=F32)


def mm_tn(a, b):
    return lax.dot_general(a, b, (((0,), (0,)), ((), ())), preferred_element_type=F32)


def row_mean(x):
    return jnp.sum(x, axis=-1, keepdims=True) * (1.0 / x.shape[-1])


def column_sum(x):
    return jnp.sum(x, axis=0, keepdims=True)


def split_norm(x):
    shifted = x - row_mean(x)
    inverse = lax.rsqrt(row_mean(shifted * shifted) + EPSILON)
    return shifted * inverse, inverse


def norm_grad(grad, unit, inverse):
    return inverse * (grad - row_mean(grad) - unit * row_mean(grad * unit))


def head_of_lane(rows):
    return lax.broadcasted_iota(jnp.int32, (rows, LANES), 1) // (LANES // HEADS)


def spread_heads(rows):
    head = head_of_lane(QWIN)
    return jnp.concatenate(
        [jnp.where(head == h, rows, jnp.zeros_like(rows)) for h in range(HEADS)], axis=0
    )


def gather_heads(rows):
    head = head_of_lane(QWIN)
    total = rows[:QWIN]
    for h in range(1, HEADS):
        total = jnp.where(head == h, rows[h * QWIN : (h + 1) * QWIN], total)
    return total


def bias_slots(row, place, rows):
    slot_lane = lax.broadcasted_iota(jnp.int32, (1, LANES), 1)
    width = LANES // HEADS
    line = jnp.zeros((1, LANES), F32)
    for h in range(HEADS):
        inside = (slot_lane // width) == h
        total = jnp.sum(jnp.where(inside, row, 0.0), axis=1, keepdims=True)
        high = total.astype(BF16).astype(F32)
        middle = (total - high).astype(BF16).astype(F32)
        low = total - high - middle
        for digit, value in enumerate((high, middle, low)):
            line = jnp.where(slot_lane % SLOT == h * 4 + digit, value, line)
    per_row = LANES // SLOT
    lane = lax.broadcasted_iota(jnp.int32, (rows, LANES), 1)
    row_index = lax.broadcasted_iota(jnp.int32, (rows, LANES), 0)
    here = (lane // SLOT == place % per_row) & (row_index == place // per_row)
    return jnp.where(here, jnp.broadcast_to(line, (rows, LANES)), 0.0)


def block_kernel(
    own_codes,
    pair_rows,
    link_rows,
    attend_gain,
    bias_row,
    transit_gain,
    state,
    project_weight,
    output_weight,
    transit_weight,
    return_weight,
    cot,
    block_out,
    back_norm,
    back_res,
    to_partner,
    to_link,
    packed_keep,
    packed_send,
    norm_ext,
    unit_ext,
    q_all,
    k_all,
    v_all,
    codes,
    probs,
    att,
    d_att,
    dq_all,
    dk_all,
    dv_all,
    grads,
    bias_acc,
):
    samples, atoms, channels = state.shape
    ext = atoms + 2 * HALO
    windows = atoms // QWIN
    place = lax.axis_index("atom")
    places = lax.axis_size("atom")
    is_odd = place % 2 == 1
    halo_rows = samples * HALO
    scale = 1.0 / math.sqrt(channels // HEADS)
    before = jnp.where(is_odd, pair_rows[...], link_rows[...])
    after = jnp.where(is_odd, link_rows[...], pair_rows[...])

    def edge_codes(part):
        high = part[halo_rows : halo_rows + 1, :].astype(F32)
        low = part[halo_rows + 1 : halo_rows + 2, :].astype(F32)
        return high * 256.0 + low

    def down_lanes(row):
        return jnp.transpose(jnp.broadcast_to(row, (LANES, LANES)))

    first_code = jnp.where(place == 0, 0.0, edge_codes(before))
    last_code = jnp.where(place == places - 1, 0.0, edge_codes(after))
    last_lane = (atoms - HALO) % LANES
    codes[0:HALO, :] = down_lanes(first_code)[last_lane : last_lane + HALO]
    for i in range(own_codes.shape[0]):
        count = min(LANES, atoms - i * LANES)
        codes[HALO + i * LANES : HALO + i * LANES + count, :] = down_lanes(own_codes[i : i + 1, :])[0:count]
    codes[HALO + atoms : ext, :] = down_lanes(last_code)[0:HALO]

    grads[...] = jnp.zeros_like(grads)
    bias_acc[...] = jnp.zeros_like(bias_acc)
    dk_all[...] = jnp.zeros_like(dk_all)
    dv_all[...] = jnp.zeros_like(dv_all)

    gain_one = attend_gain[...]
    gain_two = transit_gain[...]
    for s in range(samples):
        rows = jnp.concatenate(
            [before[s * HALO : (s + 1) * HALO], state[s], after[s * HALO : (s + 1) * HALO]], axis=0
        ).astype(F32)
        unit, _ = split_norm(rows)
        unit_ext[s] = unit
        normed = (unit * gain_one).astype(BF16)
        norm_ext[s] = normed
        projected = mm(normed, project_weight[...]).astype(BF16)
        q_all[s] = projected[HALO : HALO + atoms, :channels]
        k_all[s] = projected[:, channels : 2 * channels]
        v_all[s] = projected[:, 2 * channels :]

    def window_mask(start):
        key_code = codes[pl.ds(start, KWIN), :]
        query = codes[pl.ds(start + HALO, QWIN), :]
        query_code = jnp.transpose(jnp.concatenate([query] * HEADS, axis=0))
        return key_code, key_code == query_code

    def group_units(g):
        starts = [pl.multiple_of((g * GROUP + i) * QWIN, QWIN) for i in range(GROUP)]
        return starts, [(i, s) for i in range(GROUP) for s in range(samples)]

    def forward_group(g, carry):
        starts, units = group_units(g)
        scores = [
            mm_nt(
                k_all[s, pl.ds(starts[i], KWIN), :],
                spread_heads(q_all[s, pl.ds(starts[i], QWIN), :]),
            )
            for i, s in units
        ]
        offsets = []
        for start in starts:
            key_code, same = window_mask(start)
            offset = jnp.where(same, bias_row[...] * LOG2E, 0.0)
            offsets.append(jnp.where(key_code > 0, offset, -1e30))
        packed = []
        for (i, s), score in zip(units, scores):
            score = score * (scale * LOG2E) + offsets[i]
            weights = jnp.exp2(score - jnp.max(score, axis=0, keepdims=True))
            weights = weights * (1.0 / column_sum(weights))
            probs[(g * GROUP + i) * samples + s] = weights
            packed.append(weights.astype(BF16))
        outcomes = [
            mm_tn(weights, v_all[s, pl.ds(starts[i], KWIN), :])
            for (i, s), weights in zip(units, packed)
        ]
        for (i, s), outcome in zip(units, outcomes):
            att[s, pl.ds(starts[i], QWIN), :] = gather_heads(outcome).astype(BF16)
        return carry

    lax.fori_loop(0, windows // GROUP, forward_group, 0)

    def transition(s, gain_grad):
        attended = att[s]
        residual = (state[s].astype(F32) + mm(attended, output_weight[...])).astype(BF16)
        residual = residual.astype(F32)
        unit, inverse = split_norm(residual)
        transit_in = (unit * gain_two).astype(BF16)
        both = mm(transit_in, transit_weight[...])
        gate = both[:, :TRANS]
        up = both[:, TRANS:]
        sigmoid = 1.0 / (1.0 + jnp.exp(-gate))
        silu = gate * sigmoid
        gated = (silu * up).astype(BF16)
        block_out[s] = (residual + mm(gated, return_weight[...])).astype(BF16)
        cot16 = cot[s]
        back_gated = mm_nt(cot16, return_weight[...])
        back_gate = back_gated * up * sigmoid * (1.0 + gate * (1.0 - sigmoid))
        back_hidden = jnp.concatenate([back_gate, back_gated * silu], axis=1).astype(BF16)
        grads[pl.ds(8 * channels, TRANS), :] += mm_tn(gated, cot16)
        grad_transit = mm_tn(transit_in, back_hidden)
        for i in range(2 * TRANS // LANES):
            grads[pl.ds((4 + i) * channels, channels), :] += grad_transit[:, i * LANES : (i + 1) * LANES]
        back_transit = mm_nt(back_hidden, transit_weight[...])
        gain_grad = gain_grad + column_sum(back_transit * unit)
        back_residual = cot16.astype(F32) + norm_grad(back_transit * gain_two, unit, inverse)
        back_res[s] = back_residual
        back16 = back_residual.astype(BF16)
        grads[pl.ds(3 * channels, channels), :] += mm_tn(attended, back16)
        d_att[s] = mm_nt(back16, output_weight[...]).astype(BF16)
        return gain_grad

    zero_row = jnp.zeros((1, channels), F32)
    gain_grad_two = lax.fori_loop(0, samples, transition, zero_row)

    def backward_group(g, carry):
        starts, units = group_units(g)
        backs = [spread_heads(d_att[s, pl.ds(starts[i], QWIN), :]) for i, s in units]
        back_weights = [
            mm_nt(v_all[s, pl.ds(starts[i], KWIN), :], back) for (i, s), back in zip(units, backs)
        ]
        packed = []
        scores16 = []
        bias_parts = [None] * GROUP
        for (i, s), back_weight in zip(units, back_weights):
            weights = probs[(g * GROUP + i) * samples + s]
            weighted = weights * back_weight
            back_scores = weighted - weights * column_sum(weighted)
            bias_parts[i] = back_scores if bias_parts[i] is None else bias_parts[i] + back_scores
            packed.append(weights.astype(BF16))
            scores16.append(back_scores.astype(BF16))
        back_values = [mm(weights, back) for weights, back in zip(packed, backs)]
        back_keys = [
            mm(scores, spread_heads(q_all[s, pl.ds(starts[i], QWIN), :]))
            for (i, s), scores in zip(units, scores16)
        ]
        back_queries = [
            mm_tn(scores, k_all[s, pl.ds(starts[i], KWIN), :])
            for (i, s), scores in zip(units, scores16)
        ]
        for (i, s), value, key, query in zip(units, back_values, back_keys, back_queries):
            span = pl.ds(starts[i], KWIN)
            dv_all[s, span, :] += value
            dk_all[s, span, :] += key
            dq_all[s, pl.ds(starts[i], QWIN), :] = gather_heads(query)
        for start, bias_part in zip(starts, bias_parts):
            _, same = window_mask(start)
            bias_acc[...] += jnp.where(same, bias_part, 0.0)
        return carry

    lax.fori_loop(0, windows // GROUP, backward_group, 0)

    rim = jnp.zeros((HALO, channels), BF16)

    def projection(s, gain_grad):
        back_q = (dq_all[s] * scale).astype(BF16)
        back_q = jnp.concatenate([rim, back_q, rim], axis=0)
        back_k = (dk_all[s] * scale).astype(BF16)
        back_v = dv_all[s].astype(BF16)
        back_all = jnp.concatenate([back_q, back_k, back_v], axis=1)
        back_normed = mm_nt(back_all, project_weight[...])
        grad_project = mm_tn(norm_ext[s], back_all)
        for i in range(3):
            grads[pl.ds(i * channels, channels), :] += grad_project[:, i * LANES : (i + 1) * LANES]
        gain_grad = gain_grad + column_sum(back_normed * unit_ext[s])
        back_norm[s] = back_normed[HALO : HALO + atoms]
        rows = pl.ds(pl.multiple_of(s * HALO, HALO), HALO)
        low = back_normed[:HALO]
        high = back_normed[HALO + atoms :]
        to_partner[rows, :] = jnp.where(is_odd, low, high).astype(BF16)
        to_link[rows, :] = jnp.where(is_odd, high, low).astype(BF16)
        return gain_grad

    gain_grad_one = lax.fori_loop(0, samples, projection, zero_row)

    tail = 8 * channels + TRANS
    grads[pl.ds(tail, 1), :] = gain_grad_one
    grads[pl.ds(tail + 1, 1), :] = gain_grad_two
    slots = grads.shape[0] - tail - SLOT
    device = lax.axis_index("samp") * places + place
    grads[tail + SLOT :, :] = bias_slots(column_sum(bias_acc[...]), device, slots)
    half = packed_keep.shape[0]
    mine = place % 2
    packed_keep[...] = grads[pl.ds(pl.multiple_of(mine * half, 8), half), :].astype(BF16)
    packed_send[...] = grads[pl.ds(pl.multiple_of((1 - mine) * half, 8), half), :].astype(BF16)


def pack_kernel(valid, state, token, own_codes, partner, link, line, sem):
    samples, atoms, _ = state.shape
    odd = lax.axis_index("atom") % 2
    copies = []
    for target, start in (
        (partner, (1 - odd) * (atoms - HALO)),
        (link, odd * (atoms - HALO)),
    ):
        for s in range(samples):
            copies.append(
                pltpu.make_async_copy(
                    state.at[s, pl.ds(pl.multiple_of(start, 16), HALO)],
                    target.at[pl.ds(s * HALO, HALO)],
                    sem.at[len(copies)],
                )
            )
            copies[-1].start()
    rows = own_codes.shape[0]
    line[...] = jnp.zeros_like(line)
    line[:, :atoms] = token[...].reshape(1, atoms)
    lane = lax.broadcasted_iota(jnp.int32, (1, LANES), 1)
    codes = []
    for r in range(rows):
        limit = jnp.zeros((1, LANES), jnp.int32)
        for i in range(LANES // QWIN):
            w = r * (LANES // QWIN) + i
            if w * QWIN < atoms:
                limit = jnp.where(lane // QWIN == i, valid[w], limit)
        code = jnp.where(lane % QWIN < limit, line[:, r * LANES : (r + 1) * LANES] + 1, 0)
        codes.append(code)
        own_codes[r : r + 1, :] = code.astype(F32)
    tail_row = jnp.zeros((14, LANES), F32)
    ends = []
    for code in (codes[0], codes[-1]):
        ends.append(
            jnp.concatenate([(code // 256).astype(F32), (code % 256).astype(F32), tail_row], axis=0)
        )
    base = samples * HALO
    partner[base:, :] = jnp.where(odd == 1, ends[0], ends[1]).astype(BF16)
    link[base:, :] = jnp.where(odd == 1, ends[1], ends[0]).astype(BF16)
    for copy in copies:
        copy.wait()


def rim_kernel(state, gain, back_norm, back_res, pair_back, link_back, out):
    samples, atoms, channels = state.shape
    is_odd = lax.axis_index("atom") % 2 == 1
    from_before = jnp.where(is_odd, pair_back[...], link_back[...]).astype(F32)
    from_after = jnp.where(is_odd, link_back[...], pair_back[...]).astype(F32)
    for s in range(samples):
        grad = back_norm[s]
        part = slice(s * HALO, (s + 1) * HALO)
        grad = jnp.concatenate(
            [
                grad[:HALO] + from_before[part],
                grad[HALO : atoms - HALO],
                grad[atoms - HALO :] + from_after[part],
            ],
            axis=0,
        )
        unit, inverse = split_norm(state[s].astype(F32))
        out[s] = (back_res[s] + norm_grad(grad * gain[...], unit, inverse)).astype(BF16)


def clip_kernel(own, other, attend, project, output, bias, transit_gain, transit, back):
    channels = LANES
    first = lax.axis_index("atom") % 2 == 0
    low = jnp.where(first, own[...], other[...]).astype(F32)
    high = jnp.where(first, other[...], own[...]).astype(F32)
    total = jnp.concatenate([low, high], axis=0)
    tail = 8 * channels + TRANS
    lane = lax.broadcasted_iota(jnp.int32, (1, LANES), 1)
    digits = column_sum(total[tail + SLOT :])
    heads = jnp.zeros((1, LANES), F32)
    for h in range(HEADS):
        sum_h = jnp.sum(jnp.where((lane // 4) % 4 == h, digits, 0.0), axis=1, keepdims=True)
        heads = jnp.where(lane == h, sum_h, heads)
    plain = total[: tail + SLOT]
    squares = jnp.sum(column_sum(plain * plain) + heads * heads, axis=1, keepdims=True)
    factor = CLIP_NORM * lax.rsqrt(squares + CLIP_NORM * CLIP_NORM)
    for i in range(3):
        project[:, i * LANES : (i + 1) * LANES] = total[i * channels : (i + 1) * channels] * factor
    output[...] = total[3 * channels : 4 * channels] * factor
    for i in range(2 * TRANS // LANES):
        transit[:, i * LANES : (i + 1) * LANES] = total[(4 + i) * channels : (5 + i) * channels] * factor
    back[...] = total[8 * channels : 8 * channels + TRANS] * factor
    attend[...] = total[tail : tail + 1] * factor
    transit_gain[...] = total[tail + 1 : tail + 2] * factor
    bias[...] = (heads * factor)[:, :HEADS]


def swap(value, axis, mask):
    return lax.ppermute(value, axis, [(i, i ^ mask) for i in range(lax.axis_size(axis))])


def pair_exchange(to_partner, to_link, axis):
    size = lax.axis_size(axis)
    links = [(i, (i + 1) % size) for i in range(1, size, 2)]
    links = links + [(j, i) for i, j in links]
    return lax.ppermute(to_link, axis, links), swap(to_partner, axis, 1)


VMEM = pl.BlockSpec(memory_space=pltpu.VMEM)
SMEM = pl.BlockSpec(memory_space=pltpu.SMEM)
HBM = pl.BlockSpec(memory_space=pltpu.HBM)


def call(kernel, operands, specs, outs, scratch=(), flops=0, limit=16):
    moved = sum(x.size * x.dtype.itemsize for x in operands)
    return pl.pallas_call(
        kernel,
        out_shape=[jax.ShapeDtypeStruct(shape, dtype) for shape, dtype in outs],
        in_specs=list(specs),
        out_specs=[VMEM] * len(outs),
        scratch_shapes=list(scratch),
        cost_estimate=pl.CostEstimate(flops=flops, bytes_accessed=moved + flops // 200, transcendentals=0),
        compiler_params=pltpu.CompilerParams(vmem_limit_bytes=limit * 1024 * 1024),
    )(*operands)


def on_device(
    atom_state,
    atom_token,
    window_valid,
    attend_gain,
    project_weight,
    output_weight,
    token_bias,
    transit_gain,
    transit_weight,
    return_weight,
    cotangent,
):
    samples, atoms, channels = atom_state.shape
    ext = atoms + 2 * HALO
    windows = atoms // QWIN
    place = lax.axis_index("atom")
    devices = lax.axis_size("samp") * lax.axis_size("atom")
    slots = -(-devices * SLOT // LANES // SLOT) * SLOT
    total_rows = 8 * channels + TRANS + SLOT + slots
    half = total_rows // 2
    code_rows = -(-atoms // LANES)
    halo_rows = samples * HALO
    pack_rows = halo_rows + SLOT
    own_codes, to_partner, to_link = call(
        pack_kernel,
        (window_valid, atom_state, atom_token),
        (SMEM, HBM, VMEM),
        (
            ((code_rows, LANES), F32),
            ((pack_rows, channels), BF16),
            ((pack_rows, channels), BF16),
        ),
        (
            pltpu.VMEM((1, code_rows * LANES), jnp.int32),
            pltpu.SemaphoreType.DMA((2 * samples,)),
        ),
        flops=10_000_000_000,
    )
    link_rows, pair_rows = pair_exchange(to_partner, to_link, "atom")
    block_out, back_norm, back_res, to_partner, to_link, keep, send = call(
        block_kernel,
        (
            own_codes,
            pair_rows,
            link_rows,
            attend_gain.reshape(1, channels),
            jnp.repeat(token_bias, QWIN).reshape(1, HEADS * QWIN),
            transit_gain.reshape(1, channels),
            atom_state,
            project_weight,
            output_weight,
            transit_weight,
            return_weight,
            cotangent,
        ),
        (VMEM,) * 12,
        (
            ((samples, atoms, channels), BF16),
            ((samples, atoms, channels), F32),
            ((samples, atoms, channels), F32),
            ((halo_rows, channels), BF16),
            ((halo_rows, channels), BF16),
            ((half, channels), BF16),
            ((half, channels), BF16),
        ),
        (
            pltpu.VMEM((samples, ext, channels), BF16),
            pltpu.VMEM((samples, ext, channels), F32),
            pltpu.VMEM((samples, atoms, channels), BF16),
            pltpu.VMEM((samples, ext, channels), BF16),
            pltpu.VMEM((samples, ext, channels), BF16),
            pltpu.VMEM((ext, LANES), F32),
            pltpu.VMEM((windows * samples, KWIN, HEADS * QWIN), F32),
            pltpu.VMEM((samples, atoms, channels), BF16),
            pltpu.VMEM((samples, atoms, channels), BF16),
            pltpu.VMEM((samples, atoms, channels), F32),
            pltpu.VMEM((samples, ext, channels), F32),
            pltpu.VMEM((samples, ext, channels), F32),
            pltpu.VMEM((total_rows, channels), F32),
            pltpu.VMEM((KWIN, HEADS * QWIN), F32),
        ),
        flops=4_000_000_000,
        limit=48,
    )

    link_back, pair_back = pair_exchange(to_partner, to_link, "atom")
    cores = lax.axis_size("atom")
    part = keep + swap(send, "atom", 1)
    x_bit = (place // 2) % 2
    quarter = half // 2
    mine = lax.dynamic_slice_in_dim(part, x_bit * quarter, quarter)
    theirs = lax.dynamic_slice_in_dim(part, (1 - x_bit) * quarter, quarter)
    sums = mine + swap(theirs, "atom", 2)
    sums, link_back, pair_back = lax.optimization_barrier((sums, link_back, pair_back))
    (state_grad,) = call(
        rim_kernel,
        (atom_state, attend_gain.reshape(1, channels), back_norm, back_res, pair_back, link_back),
        (VMEM,) * 6,
        (((samples, atoms, channels), BF16),),
        flops=100_000_000,
    )
    mask = 4
    while mask < cores:
        sums = sums + swap(sums, "atom", mask)
        mask *= 2
    mask = 1
    while mask < lax.axis_size("samp"):
        sums = sums + swap(sums, "samp", mask)
        mask *= 2
    sums, state_grad = lax.optimization_barrier((sums, state_grad))
    other = swap(sums, "atom", 2)
    sums = jnp.where(
        x_bit == 0,
        jnp.concatenate([sums, other], axis=0),
        jnp.concatenate([other, sums], axis=0),
    )
    other = swap(sums, "atom", 1)
    clipped = call(
        clip_kernel,
        (sums, other),
        (VMEM,) * 2,
        (
            ((1, channels), F32),
            ((channels, 3 * channels), F32),
            ((channels, channels), F32),
            ((1, HEADS), F32),
            ((1, channels), F32),
            ((channels, 2 * TRANS), F32),
            ((TRANS, channels), F32),
        ),
    )
    return (
        block_out,
        state_grad,
        clipped[0].reshape(channels),
        clipped[1],
        clipped[2],
        clipped[3].reshape(HEADS),
        clipped[4].reshape(channels),
        clipped[5],
        clipped[6],
    )


def solution(mesh):
    return jax.shard_map(
        on_device,
        mesh=mesh,
        in_specs=(
            P("samp", "atom", None),
            P("atom"),
            P("atom"),
            P(),
            P(),
            P(),
            P(),
            P(),
            P(),
            P(),
            P("samp", "atom", None),
        ),
        out_specs=(
            P("samp", "atom", None),
            P("samp", "atom", None),
            P(),
            P(),
            P(),
            P(),
            P(),
            P(),
            P(),
        ),
        check_vma=False,
    )
```

```python
import functools
import math

import jax
import jax.numpy as jnp
from jax import lax
from jax.experimental import pallas as pl
from jax.experimental.pallas import tpu as pltpu
from jax.sharding import PartitionSpec as P

HEADS = 4
TRANS = 256
QWIN = 32
KWIN = 128
HALO = 48
EPSILON = 1e-05
CLIP_NORM = 256.0
LANES = 128
GROUP = 10
CHUNK = 2
SLOT = 16
LOG2E = 1.0 / math.log(2.0)

F32 = jnp.float32
BF16 = jnp.bfloat16


def mm(a, b):
    return lax.dot_general(a, b, (((1,), (0,)), ((), ())), preferred_element_type=F32)


def mm_nt(a, b):
    return lax.dot_general(a, b, (((1,), (1,)), ((), ())), preferred_element_type=F32)


def mm_tn(a, b):
    return lax.dot_general(a, b, (((0,), (0,)), ((), ())), preferred_element_type=F32)


def row_mean(x):
    return jnp.sum(x, axis=-1, keepdims=True) * (1.0 / x.shape[-1])


def column_sum(x):
    return jnp.sum(x, axis=0, keepdims=True)


def split_norm(x):
    shifted = x - row_mean(x)
    inverse = lax.rsqrt(row_mean(shifted * shifted) + EPSILON)
    return shifted * inverse, inverse


def norm_grad(grad, unit, inverse):
    return inverse * (grad - row_mean(grad) - unit * row_mean(grad * unit))


def head_of_lane(rows):
    return lax.broadcasted_iota(jnp.int32, (rows, LANES), 1) // (LANES // HEADS)


def spread_heads(rows):
    head = head_of_lane(QWIN)
    return jnp.concatenate(
        [jnp.where(head == h, rows, jnp.zeros_like(rows)) for h in range(HEADS)], axis=0
    )


def gather_heads(rows):
    head = head_of_lane(QWIN)
    total = rows[:QWIN]
    for h in range(1, HEADS):
        total = jnp.where(head == h, rows[h * QWIN : (h + 1) * QWIN], total)
    return total


def bias_slots(row, place, rows):
    slot_lane = lax.broadcasted_iota(jnp.int32, (1, LANES), 1)
    width = LANES // HEADS
    line = jnp.zeros((1, LANES), F32)
    for h in range(HEADS):
        inside = (slot_lane // width) == h
        total = jnp.sum(jnp.where(inside, row, 0.0), axis=1, keepdims=True)
        high = total.astype(BF16).astype(F32)
        middle = (total - high).astype(BF16).astype(F32)
        low = total - high - middle
        for digit, value in enumerate((high, middle, low)):
            line = jnp.where(slot_lane % SLOT == h * 4 + digit, value, line)
    per_row = LANES // SLOT
    lane = lax.broadcasted_iota(jnp.int32, (rows, LANES), 1)
    row_index = lax.broadcasted_iota(jnp.int32, (rows, LANES), 0)
    here = (lane // SLOT == place % per_row) & (row_index == place // per_row)
    return jnp.where(here, jnp.broadcast_to(line, (rows, LANES)), 0.0)


def block_kernel(
    own_codes,
    pair_rows,
    link_rows,
    vectors,
    state,
    project_weight,
    output_weight,
    transit_weight,
    return_weight,
    cot,
    block_out,
    back_norm,
    back_res,
    to_partner,
    to_link,
    packed_keep,
    packed_send,
    norm_ext,
    unit_ext,
    q_all,
    k_all,
    v_all,
    codes,
    probs,
    att,
    d_att,
    dq_all,
    dk_all,
    dv_all,
    grads,
    bias_acc,
):
    samples, atoms, channels = state.shape
    ext = atoms + 2 * HALO
    windows = atoms // QWIN
    place = lax.axis_index("atom")
    places = lax.axis_size("atom")
    is_odd = place % 2 == 1
    halo_rows = samples * HALO
    scale = 1.0 / math.sqrt(channels // HEADS)
    before = jnp.where(is_odd, pair_rows[...], link_rows[...])
    after = jnp.where(is_odd, link_rows[...], pair_rows[...])

    def edge_codes(part):
        high = part[halo_rows : halo_rows + 1, :].astype(F32)
        low = part[halo_rows + 1 : halo_rows + 2, :].astype(F32)
        return high * 256.0 + low

    def down_lanes(row):
        return jnp.transpose(jnp.broadcast_to(row, (LANES, LANES)))

    first_code = jnp.where(place == 0, 0.0, edge_codes(before))
    last_code = jnp.where(place == places - 1, 0.0, edge_codes(after))
    last_lane = (atoms - HALO) % LANES
    codes[0:HALO, :] = down_lanes(first_code)[last_lane : last_lane + HALO]
    for i in range(own_codes.shape[0]):
        count = min(LANES, atoms - i * LANES)
        codes[HALO + i * LANES : HALO + i * LANES + count, :] = down_lanes(own_codes[i : i + 1, :])[0:count]
    codes[HALO + atoms : ext, :] = down_lanes(last_code)[0:HALO]

    grads[...] = jnp.zeros_like(grads)
    bias_acc[...] = jnp.zeros_like(bias_acc)
    dk_all[...] = jnp.zeros_like(dk_all)
    dv_all[...] = jnp.zeros_like(dv_all)

    gain_one = vectors[0:1, :]
    gain_two = vectors[1:2, :]
    bias_row = vectors[2:3, :]
    for s in range(samples):
        rows = jnp.concatenate(
            [before[s * HALO : (s + 1) * HALO], state[s], after[s * HALO : (s + 1) * HALO]], axis=0
        ).astype(F32)
        unit, _ = split_norm(rows)
        unit_ext[s] = unit
        normed = (unit * gain_one).astype(BF16)
        norm_ext[s] = normed
        projected = mm(normed, project_weight[...]).astype(BF16)
        q_all[s] = projected[HALO : HALO + atoms, :channels]
        k_all[s] = projected[:, channels : 2 * channels]
        v_all[s] = projected[:, 2 * channels :]

    def window_mask(start):
        key_code = codes[pl.ds(start, KWIN), :]
        query = codes[pl.ds(start + HALO, QWIN), :]
        query_code = jnp.transpose(jnp.concatenate([query] * HEADS, axis=0))
        return key_code, key_code == query_code

    def group_units(g):
        starts = [pl.multiple_of((g * GROUP + i) * QWIN, QWIN) for i in range(GROUP)]
        return starts, [(i, s) for i in range(GROUP) for s in range(samples)]

    def forward_group(g, carry):
        starts, units = group_units(g)
        scores = [
            mm_nt(
                k_all[s, pl.ds(starts[i], KWIN), :],
                spread_heads(q_all[s, pl.ds(starts[i], QWIN), :]),
            )
            for i, s in units
        ]
        offsets = []
        for start in starts:
            key_code, same = window_mask(start)
            offset = jnp.where(same, bias_row * LOG2E, 0.0)
            offsets.append(jnp.where(key_code > 0, offset, -1e30))
        packed = []
        for (i, s), score in zip(units, scores):
            score = score * (scale * LOG2E) + offsets[i]
            weights = jnp.exp2(score - jnp.max(score, axis=0, keepdims=True))
            weights = weights * (1.0 / column_sum(weights))
            probs[(g * GROUP + i) * samples + s] = weights
            packed.append(weights.astype(BF16))
        outcomes = [
            mm_tn(weights, v_all[s, pl.ds(starts[i], KWIN), :])
            for (i, s), weights in zip(units, packed)
        ]
        for (i, s), outcome in zip(units, outcomes):
            att[s, pl.ds(starts[i], QWIN), :] = gather_heads(outcome).astype(BF16)
        return carry

    lax.fori_loop(0, windows // GROUP, forward_group, 0)

    chunk_rows = CHUNK * atoms

    def flat(ref, c):
        return ref[pl.ds(c * CHUNK, CHUNK)].reshape(chunk_rows, channels)

    def fill(ref, c, value):
        ref[pl.ds(c * CHUNK, CHUNK)] = value.reshape(CHUNK, atoms, channels)

    def transition(c, gain_grad):
        attended = flat(att, c)
        residual = (flat(state, c).astype(F32) + mm(attended, output_weight[...])).astype(BF16)
        residual = residual.astype(F32)
        unit, inverse = split_norm(residual)
        transit_in = (unit * gain_two).astype(BF16)
        both = mm(transit_in, transit_weight[...])
        gate = both[:, :TRANS]
        up = both[:, TRANS:]
        sigmoid = 1.0 / (1.0 + jnp.exp(-gate))
        silu = gate * sigmoid
        gated = (silu * up).astype(BF16)
        fill(block_out, c, (residual + mm(gated, return_weight[...])).astype(BF16))
        cot16 = flat(cot, c)
        back_gated = mm_nt(cot16, return_weight[...])
        back_gate = back_gated * up * sigmoid * (1.0 + gate * (1.0 - sigmoid))
        back_hidden = jnp.concatenate([back_gate, back_gated * silu], axis=1).astype(BF16)
        grads[pl.ds(8 * channels, TRANS), :] += mm_tn(gated, cot16)
        grad_transit = mm_tn(transit_in, back_hidden)
        for i in range(2 * TRANS // LANES):
            grads[pl.ds((4 + i) * channels, channels), :] += grad_transit[:, i * LANES : (i + 1) * LANES]
        back_transit = mm_nt(back_hidden, transit_weight[...])
        gain_grad = gain_grad + column_sum(back_transit * unit)
        back_residual = cot16.astype(F32) + norm_grad(back_transit * gain_two, unit, inverse)
        fill(back_res, c, back_residual)
        back16 = back_residual.astype(BF16)
        grads[pl.ds(3 * channels, channels), :] += mm_tn(attended, back16)
        fill(d_att, c, mm_nt(back16, output_weight[...]).astype(BF16))
        return gain_grad

    zero_row = jnp.zeros((1, channels), F32)
    gain_grad_two = lax.fori_loop(0, samples // CHUNK, transition, zero_row)

    def backward_group(g, carry):
        starts, units = group_units(g)
        backs = [spread_heads(d_att[s, pl.ds(starts[i], QWIN), :]) for i, s in units]
        back_weights = [
            mm_nt(v_all[s, pl.ds(starts[i], KWIN), :], back) for (i, s), back in zip(units, backs)
        ]
        packed = []
        scores16 = []
        bias_parts = [None] * GROUP
        for (i, s), back_weight in zip(units, back_weights):
            weights = probs[(g * GROUP + i) * samples + s]
            weighted = weights * back_weight
            back_scores = weighted - weights * column_sum(weighted)
            bias_parts[i] = back_scores if bias_parts[i] is None else bias_parts[i] + back_scores
            packed.append(weights.astype(BF16))
            scores16.append(back_scores.astype(BF16))
        back_values = [mm(weights, back) for weights, back in zip(packed, backs)]
        back_keys = [
            mm(scores, spread_heads(q_all[s, pl.ds(starts[i], QWIN), :]))
            for (i, s), scores in zip(units, scores16)
        ]
        back_queries = [
            mm_tn(scores, k_all[s, pl.ds(starts[i], KWIN), :])
            for (i, s), scores in zip(units, scores16)
        ]
        for (i, s), value, key, query in zip(units, back_values, back_keys, back_queries):
            span = pl.ds(starts[i], KWIN)
            dv_all[s, span, :] += value
            dk_all[s, span, :] += key
            dq_all[s, pl.ds(starts[i], QWIN), :] = gather_heads(query)
        for start, bias_part in zip(starts, bias_parts):
            _, same = window_mask(start)
            bias_acc[...] += jnp.where(same, bias_part, 0.0)
        return carry

    lax.fori_loop(0, windows // GROUP, backward_group, 0)

    rim = jnp.zeros((HALO, channels), BF16)

    def projection(c, gain_grad):
        parts = []
        for i in range(CHUNK):
            s = c * CHUNK + i
            back_q = jnp.concatenate([rim, (dq_all[s] * scale).astype(BF16), rim], axis=0)
            back_k = (dk_all[s] * scale).astype(BF16)
            parts.append(jnp.concatenate([back_q, back_k, dv_all[s].astype(BF16)], axis=1))
        back_all = jnp.concatenate(parts, axis=0)
        back_normed = mm_nt(back_all, project_weight[...])
        normed = norm_ext[pl.ds(c * CHUNK, CHUNK)].reshape(CHUNK * ext, channels)
        unit = unit_ext[pl.ds(c * CHUNK, CHUNK)].reshape(CHUNK * ext, channels)
        grad_project = mm_tn(normed, back_all)
        for i in range(3):
            grads[pl.ds(i * channels, channels), :] += grad_project[:, i * LANES : (i + 1) * LANES]
        gain_grad = gain_grad + column_sum(back_normed * unit)
        for i in range(CHUNK):
            s = c * CHUNK + i
            one = back_normed[i * ext : (i + 1) * ext]
            back_norm[s] = one[HALO : HALO + atoms]
            rows = pl.ds(pl.multiple_of(s * HALO, HALO), HALO)
            low = one[:HALO]
            high = one[HALO + atoms :]
            to_partner[rows, :] = jnp.where(is_odd, low, high).astype(BF16)
            to_link[rows, :] = jnp.where(is_odd, high, low).astype(BF16)
        return gain_grad

    gain_grad_one = lax.fori_loop(0, samples // CHUNK, projection, zero_row)

    tail = 8 * channels + TRANS
    grads[pl.ds(tail, 1), :] = gain_grad_one
    grads[pl.ds(tail + 1, 1), :] = gain_grad_two
    slots = grads.shape[0] - tail - SLOT
    device = lax.axis_index("samp") * places + place
    grads[tail + SLOT :, :] = bias_slots(column_sum(bias_acc[...]), device, slots)
    half = packed_keep.shape[0]
    mine = place % 2
    packed_keep[...] = grads[pl.ds(pl.multiple_of(mine * half, 8), half), :].astype(BF16)
    packed_send[...] = grads[pl.ds(pl.multiple_of((1 - mine) * half, 8), half), :].astype(BF16)


def lead_kernel(out):
    out[...] = jnp.zeros_like(out)


def pack_kernel(valid, blank, state, token, own_codes, partner, link, line, sem):
    samples, atoms, _ = state.shape
    odd = lax.axis_index("atom") % 2
    copies = []
    for target, start in (
        (partner, (1 - odd) * (atoms - HALO)),
        (link, odd * (atoms - HALO)),
    ):
        for s in range(samples):
            copies.append(
                pltpu.make_async_copy(
                    state.at[s, pl.ds(pl.multiple_of(start, 16), HALO)],
                    target.at[pl.ds(s * HALO, HALO)],
                    sem.at[len(copies)],
                )
            )
            copies[-1].start()
    rows = own_codes.shape[0]
    line[...] = jnp.zeros_like(line)
    line[:, :atoms] = token[...].reshape(1, atoms)
    lane = lax.broadcasted_iota(jnp.int32, (1, LANES), 1)
    codes = []
    for r in range(rows):
        limit = jnp.zeros((1, LANES), jnp.int32)
        for i in range(LANES // QWIN):
            w = r * (LANES // QWIN) + i
            if w * QWIN < atoms:
                limit = jnp.where(lane // QWIN == i, valid[w], limit)
        code = jnp.where(lane % QWIN < limit, line[:, r * LANES : (r + 1) * LANES] + 1, 0)
        codes.append(code)
        own_codes[r : r + 1, :] = code.astype(F32)
    tail_row = blank[0:14, :]
    ends = []
    for code in (codes[0], codes[-1]):
        ends.append(
            jnp.concatenate([(code // 256).astype(F32), (code % 256).astype(F32), tail_row], axis=0)
        )
    base = samples * HALO
    partner[base:, :] = jnp.where(odd == 1, ends[0], ends[1]).astype(BF16)
    link[base:, :] = jnp.where(odd == 1, ends[1], ends[0]).astype(BF16)
    for copy in copies:
        copy.wait()


def rim_kernel(state, gain, back_norm, back_res, pair_back, link_back, out):
    samples, atoms, channels = state.shape
    is_odd = lax.axis_index("atom") % 2 == 1
    from_before = jnp.where(is_odd, pair_back[...], link_back[...]).astype(F32)
    from_after = jnp.where(is_odd, link_back[...], pair_back[...]).astype(F32)
    for s in range(samples):
        grad = back_norm[s]
        part = slice(s * HALO, (s + 1) * HALO)
        grad = jnp.concatenate(
            [
                grad[:HALO] + from_before[part],
                grad[HALO : atoms - HALO],
                grad[atoms - HALO :] + from_after[part],
            ],
            axis=0,
        )
        unit, inverse = split_norm(state[s].astype(F32))
        out[s] = (back_res[s] + norm_grad(grad * gain[0:1, :], unit, inverse)).astype(BF16)


def clip_kernel(own, other, attend, project, output, bias, transit_gain, transit, back):
    channels = LANES
    first = lax.axis_index("atom") % 2 == 0
    low = jnp.where(first, own[...], other[...]).astype(F32)
    high = jnp.where(first, other[...], own[...]).astype(F32)
    total = jnp.concatenate([low, high], axis=0)
    tail = 8 * channels + TRANS
    lane = lax.broadcasted_iota(jnp.int32, (1, LANES), 1)
    digits = column_sum(total[tail + SLOT :])
    heads = jnp.zeros((1, LANES), F32)
    for h in range(HEADS):
        sum_h = jnp.sum(jnp.where((lane // 4) % 4 == h, digits, 0.0), axis=1, keepdims=True)
        heads = jnp.where(lane == h, sum_h, heads)
    plain = total[: tail + SLOT]
    squares = jnp.sum(column_sum(plain * plain) + heads * heads, axis=1, keepdims=True)
    factor = CLIP_NORM * lax.rsqrt(squares + CLIP_NORM * CLIP_NORM)
    for i in range(3):
        project[:, i * LANES : (i + 1) * LANES] = total[i * channels : (i + 1) * channels] * factor
    output[...] = total[3 * channels : 4 * channels] * factor
    for i in range(2 * TRANS // LANES):
        transit[:, i * LANES : (i + 1) * LANES] = total[(4 + i) * channels : (5 + i) * channels] * factor
    back[...] = total[8 * channels : 8 * channels + TRANS] * factor
    attend[...] = total[tail : tail + 1] * factor
    transit_gain[...] = total[tail + 1 : tail + 2] * factor
    bias[...] = (heads * factor)[:, :HEADS]


def swap(value, axis, mask):
    return lax.ppermute(value, axis, [(i, i ^ mask) for i in range(lax.axis_size(axis))])


def pair_exchange(to_partner, to_link, axis):
    size = lax.axis_size(axis)
    links = [(i, (i + 1) % size) for i in range(1, size, 2)]
    links = links + [(j, i) for i, j in links]
    return lax.ppermute(to_link, axis, links), swap(to_partner, axis, 1)


VMEM = pl.BlockSpec(memory_space=pltpu.VMEM)
SMEM = pl.BlockSpec(memory_space=pltpu.SMEM)
HBM = pl.BlockSpec(memory_space=pltpu.HBM)


def call(kernel, operands, specs, outs, scratch=(), flops=0, limit=16):
    moved = sum(x.size * x.dtype.itemsize for x in operands)
    return pl.pallas_call(
        kernel,
        out_shape=[jax.ShapeDtypeStruct(shape, dtype) for shape, dtype in outs],
        in_specs=list(specs),
        out_specs=[VMEM] * len(outs),
        scratch_shapes=list(scratch),
        cost_estimate=pl.CostEstimate(flops=flops, bytes_accessed=moved + flops // 200, transcendentals=0),
        compiler_params=pltpu.CompilerParams(vmem_limit_bytes=limit * 1024 * 1024),
    )(*operands)


def on_device(
    atom_state,
    atom_token,
    window_valid,
    attend_gain,
    project_weight,
    output_weight,
    token_bias,
    transit_gain,
    transit_weight,
    return_weight,
    cotangent,
):
    samples, atoms, channels = atom_state.shape
    ext = atoms + 2 * HALO
    windows = atoms // QWIN
    place = lax.axis_index("atom")
    devices = lax.axis_size("samp") * lax.axis_size("atom")
    slots = -(-devices * SLOT // LANES // SLOT) * SLOT
    total_rows = 8 * channels + TRANS + SLOT + slots
    half = total_rows // 2
    code_rows = -(-atoms // LANES)
    halo_rows = samples * HALO
    pack_rows = halo_rows + SLOT
    (blank,) = call(lead_kernel, (), (), (((SLOT, LANES), F32),), flops=10_000_000_000)
    own_codes, to_partner, to_link = call(
        pack_kernel,
        (window_valid, blank, atom_state, atom_token),
        (SMEM, VMEM, HBM, VMEM),
        (
            ((code_rows, LANES), F32),
            ((pack_rows, channels), BF16),
            ((pack_rows, channels), BF16),
        ),
        (
            pltpu.VMEM((1, code_rows * LANES), jnp.int32),
            pltpu.SemaphoreType.DMA((2 * samples,)),
        ),
        flops=10_000_000_000,
    )
    link_rows, pair_rows = pair_exchange(to_partner, to_link, "atom")
    vectors = jnp.stack([attend_gain, transit_gain, jnp.repeat(token_bias, QWIN)])
    block_out, back_norm, back_res, to_partner, to_link, keep, send = call(
        block_kernel,
        (
            own_codes,
            pair_rows,
            link_rows,
            vectors,
            atom_state,
            project_weight,
            output_weight,
            transit_weight,
            return_weight,
            cotangent,
        ),
        (VMEM,) * 10,
        (
            ((samples, atoms, channels), BF16),
            ((samples, atoms, channels), F32),
            ((samples, atoms, channels), F32),
            ((halo_rows, channels), BF16),
            ((halo_rows, channels), BF16),
            ((half, channels), BF16),
            ((half, channels), BF16),
        ),
        (
            pltpu.VMEM((samples, ext, channels), BF16),
            pltpu.VMEM((samples, ext, channels), F32),
            pltpu.VMEM((samples, atoms, channels), BF16),
            pltpu.VMEM((samples, ext, channels), BF16),
            pltpu.VMEM((samples, ext, channels), BF16),
            pltpu.VMEM((ext, LANES), F32),
            pltpu.VMEM((windows * samples, KWIN, HEADS * QWIN), F32),
            pltpu.VMEM((samples, atoms, channels), BF16),
            pltpu.VMEM((samples, atoms, channels), BF16),
            pltpu.VMEM((samples, atoms, channels), F32),
            pltpu.VMEM((samples, ext, channels), F32),
            pltpu.VMEM((samples, ext, channels), F32),
            pltpu.VMEM((total_rows, channels), F32),
            pltpu.VMEM((KWIN, HEADS * QWIN), F32),
        ),
        flops=4_000_000_000,
        limit=48,
    )

    link_back, pair_back = pair_exchange(to_partner, to_link, "atom")
    cores = lax.axis_size("atom")
    part = keep + swap(send, "atom", 1)
    x_bit = (place // 2) % 2
    quarter = half // 2
    mine = lax.dynamic_slice_in_dim(part, x_bit * quarter, quarter)
    theirs = lax.dynamic_slice_in_dim(part, (1 - x_bit) * quarter, quarter)
    sums = mine + swap(theirs, "atom", 2)
    mask = 4
    while mask < cores:
        sums = sums + swap(sums, "atom", mask)
        mask *= 2
    sums, link_back, pair_back = lax.optimization_barrier((sums, link_back, pair_back))
    (state_grad,) = call(
        rim_kernel,
        (atom_state, vectors, back_norm, back_res, pair_back, link_back),
        (VMEM,) * 6,
        (((samples, atoms, channels), BF16),),
        flops=100_000_000,
    )
    mask = 1
    while mask < lax.axis_size("samp"):
        sums = sums + swap(sums, "samp", mask)
        mask *= 2
    sums, state_grad = lax.optimization_barrier((sums, state_grad))
    other = swap(sums, "atom", 2)
    sums = jnp.where(
        x_bit == 0,
        jnp.concatenate([sums, other], axis=0),
        jnp.concatenate([other, sums], axis=0),
    )
    other = swap(sums, "atom", 1)
    clipped = call(
        clip_kernel,
        (sums, other),
        (VMEM,) * 2,
        (
            ((1, channels), F32),
            ((channels, 3 * channels), F32),
            ((channels, channels), F32),
            ((1, HEADS), F32),
            ((1, channels), F32),
            ((channels, 2 * TRANS), F32),
            ((TRANS, channels), F32),
        ),
    )
    return (
        block_out,
        state_grad,
        clipped[0].reshape(channels),
        clipped[1],
        clipped[2],
        clipped[3].reshape(HEADS),
        clipped[4].reshape(channels),
        clipped[5],
        clipped[6],
    )


def solution(mesh):
    return jax.shard_map(
        on_device,
        mesh=mesh,
        in_specs=(
            P("samp", "atom", None),
            P("atom"),
            P("atom"),
            P(),
            P(),
            P(),
            P(),
            P(),
            P(),
            P(),
            P("samp", "atom", None),
        ),
        out_specs=(
            P("samp", "atom", None),
            P("samp", "atom", None),
            P(),
            P(),
            P(),
            P(),
            P(),
            P(),
            P(),
        ),
        check_vma=False,
    )
```

```python
import functools
import math

import jax
import jax.numpy as jnp
from jax import lax
from jax.experimental import pallas as pl
from jax.experimental.pallas import tpu as pltpu
from jax.sharding import PartitionSpec as P

HEADS = 4
TRANS = 256
QWIN = 32
KWIN = 128
HALO = 48
EPSILON = 1e-05
CLIP_NORM = 256.0
LANES = 128
GROUP = 10
CHUNK = 2
SPAN = 2
SLOT = 16
LOG2E = 1.0 / math.log(2.0)

F32 = jnp.float32
BF16 = jnp.bfloat16


def mm(a, b):
    return lax.dot_general(a, b, (((1,), (0,)), ((), ())), preferred_element_type=F32)


def mm_nt(a, b):
    return lax.dot_general(a, b, (((1,), (1,)), ((), ())), preferred_element_type=F32)


def mm_tn(a, b):
    return lax.dot_general(a, b, (((0,), (0,)), ((), ())), preferred_element_type=F32)


def row_mean(x):
    return jnp.sum(x, axis=-1, keepdims=True) * (1.0 / x.shape[-1])


def column_sum(x):
    return jnp.sum(x, axis=0, keepdims=True)


def split_norm(x):
    shifted = x - row_mean(x)
    inverse = lax.rsqrt(row_mean(shifted * shifted) + EPSILON)
    return shifted * inverse, inverse


def norm_grad(grad, unit, inverse):
    return inverse * (grad - row_mean(grad) - unit * row_mean(grad * unit))


def head_of_lane(rows):
    return lax.broadcasted_iota(jnp.int32, (rows, LANES), 1) // (LANES // HEADS)


def spread_heads(rows):
    head = head_of_lane(QWIN)
    return jnp.concatenate(
        [jnp.where(head == h, rows, jnp.zeros_like(rows)) for h in range(HEADS)], axis=0
    )


def gather_heads(rows):
    head = head_of_lane(QWIN)
    total = rows[:QWIN]
    for h in range(1, HEADS):
        total = jnp.where(head == h, rows[h * QWIN : (h + 1) * QWIN], total)
    return total


def bias_slots(row, place, rows):
    slot_lane = lax.broadcasted_iota(jnp.int32, (1, LANES), 1)
    width = LANES // HEADS
    line = jnp.zeros((1, LANES), F32)
    for h in range(HEADS):
        inside = (slot_lane // width) == h
        total = jnp.sum(jnp.where(inside, row, 0.0), axis=1, keepdims=True)
        high = total.astype(BF16).astype(F32)
        middle = (total - high).astype(BF16).astype(F32)
        low = total - high - middle
        for digit, value in enumerate((high, middle, low)):
            line = jnp.where(slot_lane % SLOT == h * 4 + digit, value, line)
    per_row = LANES // SLOT
    lane = lax.broadcasted_iota(jnp.int32, (rows, LANES), 1)
    row_index = lax.broadcasted_iota(jnp.int32, (rows, LANES), 0)
    here = (lane // SLOT == place % per_row) & (row_index == place // per_row)
    return jnp.where(here, jnp.broadcast_to(line, (rows, LANES)), 0.0)


def block_kernel(
    own_codes,
    pair_rows,
    link_rows,
    vectors,
    state,
    project_weight,
    output_weight,
    transit_weight,
    return_weight,
    cot,
    block_out,
    back_norm,
    back_res,
    to_partner,
    to_link,
    packed_keep,
    packed_send,
    norm_ext,
    unit_ext,
    q_all,
    k_all,
    v_all,
    codes,
    probs,
    att,
    d_att,
    dq_all,
    dk_all,
    dv_all,
    grads,
    project_grads,
    total_sums,
    bias_acc,
):
    samples, atoms, channels = state.shape
    ext = atoms + 2 * HALO
    windows = atoms // QWIN
    place = lax.axis_index("atom")
    places = lax.axis_size("atom")
    is_odd = place % 2 == 1
    halo_rows = samples * HALO
    scale = 1.0 / math.sqrt(channels // HEADS)
    before = jnp.where(is_odd, pair_rows[...], link_rows[...])
    after = jnp.where(is_odd, link_rows[...], pair_rows[...])

    def edge_codes(part):
        high = part[halo_rows : halo_rows + 1, :].astype(F32)
        low = part[halo_rows + 1 : halo_rows + 2, :].astype(F32)
        return high * 256.0 + low

    def down_lanes(row):
        return jnp.transpose(jnp.broadcast_to(row, (LANES, LANES)))

    first_code = jnp.where(place == 0, 0.0, edge_codes(before))
    last_code = jnp.where(place == places - 1, 0.0, edge_codes(after))
    last_lane = (atoms - HALO) % LANES
    codes[0:HALO, :] = down_lanes(first_code)[last_lane : last_lane + HALO]
    for i in range(own_codes.shape[0]):
        count = min(LANES, atoms - i * LANES)
        codes[HALO + i * LANES : HALO + i * LANES + count, :] = down_lanes(own_codes[i : i + 1, :])[0:count]
    codes[HALO + atoms : ext, :] = down_lanes(last_code)[0:HALO]

    bias_acc[...] = jnp.zeros_like(bias_acc)
    dk_all[...] = jnp.zeros_like(dk_all)
    dv_all[...] = jnp.zeros_like(dv_all)

    gain_one = vectors[0:1, :]
    gain_two = vectors[1:2, :]
    bias_row = vectors[2:3, :]
    for s in range(samples):
        rows = jnp.concatenate(
            [before[s * HALO : (s + 1) * HALO], state[s], after[s * HALO : (s + 1) * HALO]], axis=0
        ).astype(F32)
        unit, _ = split_norm(rows)
        unit_ext[s] = unit
        normed = (unit * gain_one).astype(BF16)
        norm_ext[s] = normed
        projected = mm(normed, project_weight[...]).astype(BF16)
        q_all[s] = projected[HALO : HALO + atoms, :channels]
        k_all[s] = projected[:, channels : 2 * channels]
        v_all[s] = projected[:, 2 * channels :]

    def query_row(w):
        row, lane = divmod(w * QWIN, LANES)
        return jnp.concatenate([own_codes[row : row + 1, lane : lane + QWIN]] * HEADS, axis=1)

    query_rows = [query_row(w) for w in range(windows)]

    def window_mask(w):
        key_code = codes[w * QWIN : w * QWIN + KWIN, :]
        return key_code, key_code == query_rows[w]

    def group_units(g):
        starts = [(g * GROUP + i) * QWIN for i in range(GROUP)]
        return starts, [(i, s) for i in range(GROUP) for s in range(samples)]

    def forward_group(g, carry):
        starts, units = group_units(g)
        scores = [
            mm_nt(
                k_all[s, pl.ds(starts[i], KWIN), :],
                spread_heads(q_all[s, pl.ds(starts[i], QWIN), :]),
            )
            for i, s in units
        ]
        offsets = []
        for i in range(GROUP):
            key_code, same = window_mask(g * GROUP + i)
            offset = jnp.where(same, bias_row * LOG2E, 0.0)
            offsets.append(jnp.where(key_code > 0, offset, -1e30))
        packed = []
        for (i, s), score in zip(units, scores):
            score = score * (scale * LOG2E) + offsets[i]
            weights = jnp.exp2(score - jnp.max(score, axis=0, keepdims=True))
            weights = weights * (1.0 / column_sum(weights))
            probs[(g * GROUP + i) * samples + s] = weights
            packed.append(weights.astype(BF16))
        outcomes = [
            mm_tn(weights, v_all[s, pl.ds(starts[i], KWIN), :])
            for (i, s), weights in zip(units, packed)
        ]
        for (i, s), outcome in zip(units, outcomes):
            att[s, pl.ds(starts[i], QWIN), :] = gather_heads(outcome).astype(BF16)
        return carry

    for g in range(windows // GROUP):
        forward_group(g, 0)

    chunk_rows = CHUNK * atoms

    def flat(ref, c):
        return ref[pl.ds(c * CHUNK, CHUNK)].reshape(chunk_rows, channels)

    def fill(ref, c, value):
        ref[pl.ds(c * CHUNK, CHUNK)] = value.reshape(CHUNK, atoms, channels)

    def transition(c, gain_grad):
        attended = flat(att, c)
        residual = (flat(state, c).astype(F32) + mm(attended, output_weight[...])).astype(BF16)
        residual = residual.astype(F32)
        unit, inverse = split_norm(residual)
        transit_in = (unit * gain_two).astype(BF16)
        both = mm(transit_in, transit_weight[...])
        gate = both[:, :TRANS]
        up = both[:, TRANS:]
        sigmoid = 1.0 / (1.0 + jnp.exp(-gate))
        silu = gate * sigmoid
        gated = (silu * up).astype(BF16)
        fill(block_out, c, (residual + mm(gated, return_weight[...])).astype(BF16))
        cot16 = flat(cot, c)
        back_gated = mm_nt(cot16, return_weight[...])
        back_gate = back_gated * up * sigmoid * (1.0 + gate * (1.0 - sigmoid))
        back_hidden = jnp.concatenate([back_gate, back_gated * silu], axis=1).astype(BF16)
        grads[c, pl.ds(8 * channels, TRANS), :] = mm_tn(gated, cot16)
        grad_transit = mm_tn(transit_in, back_hidden)
        for i in range(2 * TRANS // LANES):
            grads[c, pl.ds((4 + i) * channels, channels), :] = grad_transit[:, i * LANES : (i + 1) * LANES]
        back_transit = mm_nt(back_hidden, transit_weight[...])
        gain_grad = gain_grad + column_sum(back_transit * unit)
        back_residual = cot16.astype(F32) + norm_grad(back_transit * gain_two, unit, inverse)
        fill(back_res, c, back_residual)
        back16 = back_residual.astype(BF16)
        grads[c, pl.ds(3 * channels, channels), :] = mm_tn(attended, back16)
        fill(d_att, c, mm_nt(back16, output_weight[...]).astype(BF16))
        return gain_grad

    zero_row = jnp.zeros((1, channels), F32)
    gain_grad_two = zero_row
    for c in range(samples // CHUNK):
        gain_grad_two = transition(c, gain_grad_two)

    def backward_group(g, carry):
        starts, units = group_units(g)
        backs = [spread_heads(d_att[s, pl.ds(starts[i], QWIN), :]) for i, s in units]
        back_weights = [
            mm_nt(v_all[s, pl.ds(starts[i], KWIN), :], back) for (i, s), back in zip(units, backs)
        ]
        packed = []
        scores16 = []
        bias_parts = [None] * GROUP
        for (i, s), back_weight in zip(units, back_weights):
            weights = probs[(g * GROUP + i) * samples + s]
            weighted = weights * back_weight
            back_scores = weighted - weights * column_sum(weighted)
            bias_parts[i] = back_scores if bias_parts[i] is None else bias_parts[i] + back_scores
            packed.append(weights.astype(BF16))
            scores16.append(back_scores.astype(BF16))
        back_values = [mm(weights, back) for weights, back in zip(packed, backs)]
        back_keys = [
            mm(scores, spread_heads(q_all[s, pl.ds(starts[i], QWIN), :]))
            for (i, s), scores in zip(units, scores16)
        ]
        back_queries = [
            mm_tn(scores, k_all[s, pl.ds(starts[i], KWIN), :])
            for (i, s), scores in zip(units, scores16)
        ]
        for (i, s), value, key, query in zip(units, back_values, back_keys, back_queries):
            span = pl.ds(starts[i], KWIN)
            dv_all[s, span, :] += value
            dk_all[s, span, :] += key
            dq_all[s, pl.ds(starts[i], QWIN), :] = gather_heads(query)
        for i, bias_part in enumerate(bias_parts):
            _, same = window_mask(g * GROUP + i)
            bias_acc[...] += jnp.where(same, bias_part, 0.0)
        return carry

    for g in range(windows // GROUP):
        backward_group(g, 0)

    rim = jnp.zeros((HALO, channels), BF16)

    def projection(c, gain_grad):
        parts = []
        for i in range(SPAN):
            s = c * SPAN + i
            back_q = jnp.concatenate([rim, (dq_all[s] * scale).astype(BF16), rim], axis=0)
            back_k = (dk_all[s] * scale).astype(BF16)
            parts.append(jnp.concatenate([back_q, back_k, dv_all[s].astype(BF16)], axis=1))
        back_all = jnp.concatenate(parts, axis=0)
        back_normed = mm_nt(back_all, project_weight[...])
        normed = norm_ext[pl.ds(c * SPAN, SPAN)].reshape(SPAN * ext, channels)
        unit = unit_ext[pl.ds(c * SPAN, SPAN)].reshape(SPAN * ext, channels)
        grad_project = mm_tn(normed, back_all)
        for i in range(3):
            project_grads[c, pl.ds(i * channels, channels), :] = grad_project[:, i * LANES : (i + 1) * LANES]
        gain_grad = gain_grad + column_sum(back_normed * unit)
        for i in range(SPAN):
            s = c * SPAN + i
            one = back_normed[i * ext : (i + 1) * ext]
            back_norm[s] = one[HALO : HALO + atoms]
            rows = pl.ds(pl.multiple_of(s * HALO, HALO), HALO)
            low = one[:HALO]
            high = one[HALO + atoms :]
            to_partner[rows, :] = jnp.where(is_odd, low, high).astype(BF16)
            to_link[rows, :] = jnp.where(is_odd, high, low).astype(BF16)
        return gain_grad

    gain_grad_one = zero_row
    for c in range(samples // SPAN):
        gain_grad_one = projection(c, gain_grad_one)

    tail = 8 * channels + TRANS
    lead = 3 * channels

    def add_up(parts, start, stop):
        total = parts[0, start:stop, :]
        for c in range(1, parts.shape[0]):
            total = total + parts[c, start:stop, :]
        return total

    slots = total_sums.shape[0] - tail - SLOT
    device = lax.axis_index("samp") * places + place
    total_sums[:lead, :] = add_up(project_grads, 0, lead)
    total_sums[lead:tail, :] = add_up(grads, lead, tail)
    total_sums[tail : tail + SLOT, :] = jnp.concatenate(
        [gain_grad_one, gain_grad_two, jnp.zeros((SLOT - 2, channels), F32)], axis=0
    )
    total_sums[tail + SLOT :, :] = bias_slots(column_sum(bias_acc[...]), device, slots)
    half = packed_keep.shape[0]
    mine = place % 2
    packed_keep[...] = total_sums[pl.ds(pl.multiple_of(mine * half, 8), half), :].astype(BF16)
    packed_send[...] = total_sums[pl.ds(pl.multiple_of((1 - mine) * half, 8), half), :].astype(BF16)


def lead_kernel(out):
    out[...] = jnp.zeros_like(out)


def pack_kernel(valid, blank, state, token, own_codes, partner, link, line, sem):
    samples, atoms, _ = state.shape
    odd = lax.axis_index("atom") % 2
    copies = []
    for target, start in (
        (partner, (1 - odd) * (atoms - HALO)),
        (link, odd * (atoms - HALO)),
    ):
        for s in range(samples):
            copies.append(
                pltpu.make_async_copy(
                    state.at[s, pl.ds(pl.multiple_of(start, 16), HALO)],
                    target.at[pl.ds(s * HALO, HALO)],
                    sem.at[len(copies)],
                )
            )
            copies[-1].start()
    rows = own_codes.shape[0]
    line[...] = jnp.zeros_like(line)
    line[:, :atoms] = token[...].reshape(1, atoms)
    lane = lax.broadcasted_iota(jnp.int32, (1, LANES), 1)
    codes = []
    for r in range(rows):
        limit = jnp.zeros((1, LANES), jnp.int32)
        for i in range(LANES // QWIN):
            w = r * (LANES // QWIN) + i
            if w * QWIN < atoms:
                limit = jnp.where(lane // QWIN == i, valid[w], limit)
        code = jnp.where(lane % QWIN < limit, line[:, r * LANES : (r + 1) * LANES] + 1, 0)
        codes.append(code)
        own_codes[r : r + 1, :] = code.astype(F32)
    tail_row = blank[0:14, :]
    ends = []
    for code in (codes[0], codes[-1]):
        ends.append(
            jnp.concatenate([(code // 256).astype(F32), (code % 256).astype(F32), tail_row], axis=0)
        )
    base = samples * HALO
    partner[base:, :] = jnp.where(odd == 1, ends[0], ends[1]).astype(BF16)
    link[base:, :] = jnp.where(odd == 1, ends[1], ends[0]).astype(BF16)
    for copy in copies:
        copy.wait()


def rim_kernel(state, gain, back_norm, back_res, pair_back, link_back, out):
    samples, atoms, channels = state.shape
    is_odd = lax.axis_index("atom") % 2 == 1
    from_before = jnp.where(is_odd, pair_back[...], link_back[...]).astype(F32)
    from_after = jnp.where(is_odd, link_back[...], pair_back[...]).astype(F32)
    for s in range(samples):
        grad = back_norm[s]
        part = slice(s * HALO, (s + 1) * HALO)
        grad = jnp.concatenate(
            [
                grad[:HALO] + from_before[part],
                grad[HALO : atoms - HALO],
                grad[atoms - HALO :] + from_after[part],
            ],
            axis=0,
        )
        unit, inverse = split_norm(state[s].astype(F32))
        out[s] = (back_res[s] + norm_grad(grad * gain[0:1, :], unit, inverse)).astype(BF16)


def clip_kernel(own, other, attend, project, output, bias, transit_gain, transit, back):
    channels = LANES
    first = lax.axis_index("atom") % 2 == 0
    low = jnp.where(first, own[...], other[...]).astype(F32)
    high = jnp.where(first, other[...], own[...]).astype(F32)
    total = jnp.concatenate([low, high], axis=0)
    tail = 8 * channels + TRANS
    lane = lax.broadcasted_iota(jnp.int32, (1, LANES), 1)
    digits = column_sum(total[tail + SLOT :])
    heads = jnp.zeros((1, LANES), F32)
    for h in range(HEADS):
        sum_h = jnp.sum(jnp.where((lane // 4) % 4 == h, digits, 0.0), axis=1, keepdims=True)
        heads = jnp.where(lane == h, sum_h, heads)
    plain = total[: tail + SLOT]
    squares = jnp.sum(column_sum(plain * plain) + heads * heads, axis=1, keepdims=True)
    factor = CLIP_NORM * lax.rsqrt(squares + CLIP_NORM * CLIP_NORM)
    for i in range(3):
        project[:, i * LANES : (i + 1) * LANES] = total[i * channels : (i + 1) * channels] * factor
    output[...] = total[3 * channels : 4 * channels] * factor
    for i in range(2 * TRANS // LANES):
        transit[:, i * LANES : (i + 1) * LANES] = total[(4 + i) * channels : (5 + i) * channels] * factor
    back[...] = total[8 * channels : 8 * channels + TRANS] * factor
    attend[...] = total[tail : tail + 1] * factor
    transit_gain[...] = total[tail + 1 : tail + 2] * factor
    bias[...] = (heads * factor)[:, :HEADS]


def swap(value, axis, mask):
    return lax.ppermute(value, axis, [(i, i ^ mask) for i in range(lax.axis_size(axis))])


def pair_exchange(to_partner, to_link, axis):
    size = lax.axis_size(axis)
    links = [(i, (i + 1) % size) for i in range(1, size, 2)]
    links = links + [(j, i) for i, j in links]
    return lax.ppermute(to_link, axis, links), swap(to_partner, axis, 1)


VMEM = pl.BlockSpec(memory_space=pltpu.VMEM)
SMEM = pl.BlockSpec(memory_space=pltpu.SMEM)
HBM = pl.BlockSpec(memory_space=pltpu.HBM)


def call(kernel, operands, specs, outs, scratch=(), flops=0, limit=16):
    moved = sum(x.size * x.dtype.itemsize for x in operands)
    return pl.pallas_call(
        kernel,
        out_shape=[jax.ShapeDtypeStruct(shape, dtype) for shape, dtype in outs],
        in_specs=list(specs),
        out_specs=[VMEM] * len(outs),
        scratch_shapes=list(scratch),
        cost_estimate=pl.CostEstimate(flops=flops, bytes_accessed=moved + flops // 200, transcendentals=0),
        compiler_params=pltpu.CompilerParams(vmem_limit_bytes=limit * 1024 * 1024),
    )(*operands)


def on_device(
    atom_state,
    atom_token,
    window_valid,
    attend_gain,
    project_weight,
    output_weight,
    token_bias,
    transit_gain,
    transit_weight,
    return_weight,
    cotangent,
):
    samples, atoms, channels = atom_state.shape
    ext = atoms + 2 * HALO
    windows = atoms // QWIN
    place = lax.axis_index("atom")
    devices = lax.axis_size("samp") * lax.axis_size("atom")
    slots = -(-devices * SLOT // LANES // SLOT) * SLOT
    total_rows = 8 * channels + TRANS + SLOT + slots
    half = total_rows // 2
    code_rows = -(-atoms // LANES)
    halo_rows = samples * HALO
    pack_rows = halo_rows + SLOT
    (blank,) = call(lead_kernel, (), (), (((SLOT, LANES), F32),), flops=10_000_000_000)
    own_codes, to_partner, to_link = call(
        pack_kernel,
        (window_valid, blank, atom_state, atom_token),
        (SMEM, VMEM, HBM, VMEM),
        (
            ((code_rows, LANES), F32),
            ((pack_rows, channels), BF16),
            ((pack_rows, channels), BF16),
        ),
        (
            pltpu.VMEM((1, code_rows * LANES), jnp.int32),
            pltpu.SemaphoreType.DMA((2 * samples,)),
        ),
        flops=10_000_000_000,
    )
    link_rows, pair_rows = pair_exchange(to_partner, to_link, "atom")
    vectors = jnp.stack([attend_gain, transit_gain, jnp.repeat(token_bias, QWIN)])
    block_out, back_norm, back_res, to_partner, to_link, keep, send = call(
        block_kernel,
        (
            own_codes,
            pair_rows,
            link_rows,
            vectors,
            atom_state,
            project_weight,
            output_weight,
            transit_weight,
            return_weight,
            cotangent,
        ),
        (VMEM,) * 10,
        (
            ((samples, atoms, channels), BF16),
            ((samples, atoms, channels), F32),
            ((samples, atoms, channels), F32),
            ((halo_rows, channels), BF16),
            ((halo_rows, channels), BF16),
            ((half, channels), BF16),
            ((half, channels), BF16),
        ),
        (
            pltpu.VMEM((samples, ext, channels), BF16),
            pltpu.VMEM((samples, ext, channels), F32),
            pltpu.VMEM((samples, atoms, channels), BF16),
            pltpu.VMEM((samples, ext, channels), BF16),
            pltpu.VMEM((samples, ext, channels), BF16),
            pltpu.VMEM((ext, LANES), F32),
            pltpu.VMEM((windows * samples, KWIN, HEADS * QWIN), F32),
            pltpu.VMEM((samples, atoms, channels), BF16),
            pltpu.VMEM((samples, atoms, channels), BF16),
            pltpu.VMEM((samples, atoms, channels), F32),
            pltpu.VMEM((samples, ext, channels), F32),
            pltpu.VMEM((samples, ext, channels), F32),
            pltpu.VMEM((samples // CHUNK, 8 * channels + TRANS, channels), F32),
            pltpu.VMEM((samples // SPAN, 3 * channels, channels), F32),
            pltpu.VMEM((total_rows, channels), F32),
            pltpu.VMEM((KWIN, HEADS * QWIN), F32),
        ),
        flops=4_000_000_000,
        limit=48,
    )

    link_back, pair_back = pair_exchange(to_partner, to_link, "atom")
    cores = lax.axis_size("atom")
    part = keep + swap(send, "atom", 1)
    x_bit = (place // 2) % 2
    quarter = half // 2
    mine = lax.dynamic_slice_in_dim(part, x_bit * quarter, quarter)
    theirs = lax.dynamic_slice_in_dim(part, (1 - x_bit) * quarter, quarter)
    sums = mine + swap(theirs, "atom", 2)
    mask = 4
    while mask < cores:
        sums = sums + swap(sums, "atom", mask)
        mask *= 2
    sums, link_back, pair_back = lax.optimization_barrier((sums, link_back, pair_back))
    (state_grad,) = call(
        rim_kernel,
        (atom_state, vectors, back_norm, back_res, pair_back, link_back),
        (VMEM,) * 6,
        (((samples, atoms, channels), BF16),),
        flops=100_000_000,
    )
    mask = 1
    while mask < lax.axis_size("samp"):
        sums = sums + swap(sums, "samp", mask)
        mask *= 2
    sums, state_grad = lax.optimization_barrier((sums, state_grad))
    other = swap(sums, "atom", 2)
    sums = jnp.where(
        x_bit == 0,
        jnp.concatenate([sums, other], axis=0),
        jnp.concatenate([other, sums], axis=0),
    )
    other = swap(sums, "atom", 1)
    clipped = call(
        clip_kernel,
        (sums, other),
        (VMEM,) * 2,
        (
            ((1, channels), F32),
            ((channels, 3 * channels), F32),
            ((channels, channels), F32),
            ((1, HEADS), F32),
            ((1, channels), F32),
            ((channels, 2 * TRANS), F32),
            ((TRANS, channels), F32),
        ),
    )
    return (
        block_out,
        state_grad,
        clipped[0].reshape(channels),
        clipped[1],
        clipped[2],
        clipped[3].reshape(HEADS),
        clipped[4].reshape(channels),
        clipped[5],
        clipped[6],
    )


def solution(mesh):
    return jax.shard_map(
        on_device,
        mesh=mesh,
        in_specs=(
            P("samp", "atom", None),
            P("atom"),
            P("atom"),
            P(),
            P(),
            P(),
            P(),
            P(),
            P(),
            P(),
            P("samp", "atom", None),
        ),
        out_specs=(
            P("samp", "atom", None),
            P("samp", "atom", None),
            P(),
            P(),
            P(),
            P(),
            P(),
            P(),
            P(),
        ),
        check_vma=False,
    )
```

```python
import functools
import math

import jax
import jax.numpy as jnp
from jax import lax
from jax.experimental import pallas as pl
from jax.experimental.pallas import tpu as pltpu
from jax.sharding import PartitionSpec as P

HEADS = 4
TRANS = 256
QWIN = 32
KWIN = 128
HALO = 48
EPSILON = 1e-05
CLIP_NORM = 256.0
LANES = 128
GROUP = 10
CHUNK = 2
SPAN = 2
SLOT = 16
LOG2E = 1.0 / math.log(2.0)

F32 = jnp.float32
BF16 = jnp.bfloat16


def mm(a, b):
    return lax.dot_general(a, b, (((1,), (0,)), ((), ())), preferred_element_type=F32)


def mm_nt(a, b):
    return lax.dot_general(a, b, (((1,), (1,)), ((), ())), preferred_element_type=F32)


def mm_tn(a, b):
    return lax.dot_general(a, b, (((0,), (0,)), ((), ())), preferred_element_type=F32)


def row_mean(x):
    return jnp.sum(x, axis=-1, keepdims=True) * (1.0 / x.shape[-1])


def column_sum(x):
    return jnp.sum(x, axis=0, keepdims=True)


def split_norm(x):
    shifted = x - row_mean(x)
    inverse = lax.rsqrt(row_mean(shifted * shifted) + EPSILON)
    return shifted * inverse, inverse


def norm_grad(grad, unit, inverse):
    return inverse * (grad - row_mean(grad) - unit * row_mean(grad * unit))


def head_of_lane(rows):
    return lax.broadcasted_iota(jnp.int32, (rows, LANES), 1) // (LANES // HEADS)


def spread_heads(rows):
    head = head_of_lane(QWIN)
    return jnp.concatenate(
        [jnp.where(head == h, rows, jnp.zeros_like(rows)) for h in range(HEADS)], axis=0
    )


def gather_heads(rows):
    head = head_of_lane(QWIN)
    total = rows[:QWIN]
    for h in range(1, HEADS):
        total = jnp.where(head == h, rows[h * QWIN : (h + 1) * QWIN], total)
    return total


def bias_slots(row, place, rows):
    slot_lane = lax.broadcasted_iota(jnp.int32, (1, LANES), 1)
    width = LANES // HEADS
    line = jnp.zeros((1, LANES), F32)
    for h in range(HEADS):
        inside = (slot_lane // width) == h
        total = jnp.sum(jnp.where(inside, row, 0.0), axis=1, keepdims=True)
        high = total.astype(BF16).astype(F32)
        middle = (total - high).astype(BF16).astype(F32)
        low = total - high - middle
        for digit, value in enumerate((high, middle, low)):
            line = jnp.where(slot_lane % SLOT == h * 4 + digit, value, line)
    per_row = LANES // SLOT
    lane = lax.broadcasted_iota(jnp.int32, (rows, LANES), 1)
    row_index = lax.broadcasted_iota(jnp.int32, (rows, LANES), 0)
    here = (lane // SLOT == place % per_row) & (row_index == place // per_row)
    return jnp.where(here, jnp.broadcast_to(line, (rows, LANES)), 0.0)


def is_inner(w, atoms):
    return w * QWIN >= HALO and w * QWIN + KWIN - HALO <= atoms


def down_lanes(row):
    return jnp.transpose(jnp.broadcast_to(row, (LANES, LANES)))


def fill_own_codes(codes, own_codes, atoms):
    for i in range(own_codes.shape[0]):
        count = min(LANES, atoms - i * LANES)
        start = HALO + i * LANES
        codes[start : start + count, :] = down_lanes(own_codes[i : i + 1, :])[0:count]


def query_row(own_codes, w):
    row, lane = divmod(w * QWIN, LANES)
    return jnp.concatenate([own_codes[row : row + 1, lane : lane + QWIN]] * HEADS, axis=1)


def window_mask(codes, own_codes, w):
    key_code = codes[w * QWIN : w * QWIN + KWIN, :]
    return key_code, key_code == query_row(own_codes, w)


def attend_windows(picked, samples, query_of, key_of, value_of, codes, own_codes, bias_row, probs, att):
    scale = 1.0 / math.sqrt(LANES // HEADS)
    units = [(w, s) for w in picked for s in range(samples)]
    scores = [mm_nt(key_of(s, w), spread_heads(query_of(s, w))) for w, s in units]
    offsets = {}
    for w in picked:
        key_code, same = window_mask(codes, own_codes, w)
        offset = jnp.where(same, bias_row * LOG2E, 0.0)
        offsets[w] = jnp.where(key_code > 0, offset, -1e30)
    packed = []
    for (w, s), score in zip(units, scores):
        score = score * (scale * LOG2E) + offsets[w]
        weights = jnp.exp2(score - jnp.max(score, axis=0, keepdims=True))
        weights = weights * (1.0 / column_sum(weights))
        probs[w * samples + s] = weights
        packed.append(weights.astype(BF16))
    outcomes = [mm_tn(weights, value_of(s, w)) for (w, s), weights in zip(units, packed)]
    for (w, s), outcome in zip(units, outcomes):
        att[s, w * QWIN : (w + 1) * QWIN, :] = gather_heads(outcome).astype(BF16)


def inner_kernel(
    own_codes, vectors, state, project_weight, norm_own, unit_own, q_own, k_own, v_own, probs, att, codes
):
    samples, atoms, channels = state.shape
    fill_own_codes(codes, own_codes, atoms)
    for s in range(samples):
        unit, _ = split_norm(state[s].astype(F32))
        unit_own[s] = unit
        normed = (unit * vectors[0:1, :]).astype(BF16)
        norm_own[s] = normed
        projected = mm(normed, project_weight[...]).astype(BF16)
        q_own[s] = projected[:, :channels]
        k_own[s] = projected[:, channels : 2 * channels]
        v_own[s] = projected[:, 2 * channels :]

    def own_window(ref, s, w):
        return ref[s, w * QWIN - HALO : w * QWIN - HALO + KWIN, :]

    attend_windows(
        [w for w in range(atoms // QWIN) if is_inner(w, atoms)],
        samples,
        lambda s, w: q_own[s, w * QWIN : (w + 1) * QWIN, :],
        lambda s, w: own_window(k_own, s, w),
        lambda s, w: own_window(v_own, s, w),
        codes,
        own_codes,
        vectors[2:3, :],
        probs,
        att,
    )


def block_kernel(
    own_codes,
    pair_rows,
    link_rows,
    vectors,
    norm_own,
    unit_own,
    q_all,
    k_own,
    v_own,
    probs_own,
    att_own,
    state,
    project_weight,
    output_weight,
    transit_weight,
    return_weight,
    cot,
    block_out,
    back_norm,
    back_res,
    to_partner,
    to_link,
    packed_keep,
    packed_send,
    norm_rim,
    unit_rim,
    k_all,
    v_all,
    codes,
    probs,
    att,
    d_att,
    dq_all,
    dk_all,
    dv_all,
    grads,
    project_grads,
    total_sums,
    bias_acc,
):
    samples, atoms, channels = state.shape
    ext = atoms + 2 * HALO
    windows = atoms // QWIN
    place = lax.axis_index("atom")
    places = lax.axis_size("atom")
    is_odd = place % 2 == 1
    halo_rows = samples * HALO
    scale = 1.0 / math.sqrt(channels // HEADS)
    before = jnp.where(is_odd, pair_rows[...], link_rows[...])
    after = jnp.where(is_odd, link_rows[...], pair_rows[...])

    def edge_codes(part):
        high = part[halo_rows : halo_rows + 1, :].astype(F32)
        low = part[halo_rows + 1 : halo_rows + 2, :].astype(F32)
        return high * 256.0 + low

    first_code = jnp.where(place == 0, 0.0, edge_codes(before))
    last_code = jnp.where(place == places - 1, 0.0, edge_codes(after))
    last_lane = (atoms - HALO) % LANES
    codes[0:HALO, :] = down_lanes(first_code)[last_lane : last_lane + HALO]
    fill_own_codes(codes, own_codes, atoms)
    codes[HALO + atoms : ext, :] = down_lanes(last_code)[0:HALO]

    bias_acc[...] = jnp.zeros_like(bias_acc)
    dk_all[...] = jnp.zeros_like(dk_all)
    dv_all[...] = jnp.zeros_like(dv_all)

    gain_one = vectors[0:1, :]
    gain_two = vectors[1:2, :]
    bias_row = vectors[2:3, :]
    keep_rows = KWIN - QWIN + HALO
    keep_rows = min(atoms, keep_rows + QWIN)
    both_rims = jnp.concatenate([before[:halo_rows], after[:halo_rows]], axis=0).astype(F32)
    unit, _ = split_norm(both_rims)
    unit_rim[...] = unit
    normed = (unit * gain_one).astype(BF16)
    norm_rim[...] = normed
    rim_pairs = mm(normed, project_weight[:, channels:]).astype(BF16)
    for ref, own, column in ((k_all, k_own, 0), (v_all, v_own, channels)):
        part = rim_pairs[:, column : column + channels]
        for s in range(samples):
            ref[s, :HALO, :] = part[s * HALO : (s + 1) * HALO]
            ref[s, HALO : HALO + keep_rows, :] = own[s, :keep_rows, :]
            ref[s, HALO + atoms - keep_rows : HALO + atoms, :] = own[s, atoms - keep_rows :, :]
            ref[s, HALO + atoms :, :] = part[halo_rows + s * HALO : halo_rows + (s + 1) * HALO]

    def pair_window(ext_ref, own_ref, s, w):
        if is_inner(w, atoms):
            return own_ref[s, w * QWIN - HALO : w * QWIN - HALO + KWIN, :]
        return ext_ref[s, w * QWIN : w * QWIN + KWIN, :]

    def key_of(s, w):
        return pair_window(k_all, k_own, s, w)

    def value_of(s, w):
        return pair_window(v_all, v_own, s, w)

    def query_of(s, w):
        return q_all[s, w * QWIN : (w + 1) * QWIN, :]

    def prob_of(s, w):
        return (probs_own if is_inner(w, atoms) else probs)[w * samples + s]

    outer = [w for w in range(windows) if not is_inner(w, atoms)]
    attend_windows(
        outer, samples, query_of, key_of, value_of, codes, own_codes, bias_row, probs, att
    )
    for s in range(samples):
        for w in range(windows):
            if is_inner(w, atoms):
                span = slice(w * QWIN, (w + 1) * QWIN)
                att[s, span, :] = att_own[s, span, :]

    def group_units(g):
        starts = [(g * GROUP + i) * QWIN for i in range(GROUP)]
        return starts, [(i, s) for i in range(GROUP) for s in range(samples)]

    chunk_rows = CHUNK * atoms

    def flat(ref, c):
        return ref[pl.ds(c * CHUNK, CHUNK)].reshape(chunk_rows, channels)

    def fill(ref, c, value):
        ref[pl.ds(c * CHUNK, CHUNK)] = value.reshape(CHUNK, atoms, channels)

    def transition(c, gain_grad):
        attended = flat(att, c)
        residual = (flat(state, c).astype(F32) + mm(attended, output_weight[...])).astype(BF16)
        residual = residual.astype(F32)
        unit, inverse = split_norm(residual)
        transit_in = (unit * gain_two).astype(BF16)
        both = mm(transit_in, transit_weight[...])
        gate = both[:, :TRANS]
        up = both[:, TRANS:]
        sigmoid = 1.0 / (1.0 + jnp.exp(-gate))
        silu = gate * sigmoid
        gated = (silu * up).astype(BF16)
        fill(block_out, c, (residual + mm(gated, return_weight[...])).astype(BF16))
        cot16 = flat(cot, c)
        back_gated = mm_nt(cot16, return_weight[...])
        back_gate = back_gated * up * sigmoid * (1.0 + gate * (1.0 - sigmoid))
        back_hidden = jnp.concatenate([back_gate, back_gated * silu], axis=1).astype(BF16)
        grads[c, pl.ds(8 * channels, TRANS), :] = mm_tn(gated, cot16)
        grad_transit = mm_tn(transit_in, back_hidden)
        for i in range(2 * TRANS // LANES):
            grads[c, pl.ds((4 + i) * channels, channels), :] = grad_transit[:, i * LANES : (i + 1) * LANES]
        back_transit = mm_nt(back_hidden, transit_weight[...])
        gain_grad = gain_grad + column_sum(back_transit * unit)
        back_residual = cot16.astype(F32) + norm_grad(back_transit * gain_two, unit, inverse)
        fill(back_res, c, back_residual)
        back16 = back_residual.astype(BF16)
        grads[c, pl.ds(3 * channels, channels), :] = mm_tn(attended, back16)
        fill(d_att, c, mm_nt(back16, output_weight[...]).astype(BF16))
        return gain_grad

    zero_row = jnp.zeros((1, channels), F32)
    gain_grad_two = zero_row
    for c in range(samples // CHUNK):
        gain_grad_two = transition(c, gain_grad_two)

    def backward_group(g, carry):
        starts, units = group_units(g)
        backs = [spread_heads(d_att[s, pl.ds(starts[i], QWIN), :]) for i, s in units]
        back_weights = [
            mm_nt(value_of(s, g * GROUP + i), back) for (i, s), back in zip(units, backs)
        ]
        packed = []
        scores16 = []
        bias_parts = [None] * GROUP
        for (i, s), back_weight in zip(units, back_weights):
            weights = prob_of(s, g * GROUP + i)
            weighted = weights * back_weight
            back_scores = weighted - weights * column_sum(weighted)
            bias_parts[i] = back_scores if bias_parts[i] is None else bias_parts[i] + back_scores
            packed.append(weights.astype(BF16))
            scores16.append(back_scores.astype(BF16))
        back_values = [mm(weights, back) for weights, back in zip(packed, backs)]
        back_keys = [
            mm(scores, spread_heads(q_all[s, pl.ds(starts[i], QWIN), :]))
            for (i, s), scores in zip(units, scores16)
        ]
        back_queries = [
            mm_tn(scores, key_of(s, g * GROUP + i))
            for (i, s), scores in zip(units, scores16)
        ]
        for (i, s), value, key, query in zip(units, back_values, back_keys, back_queries):
            span = pl.ds(starts[i], KWIN)
            dv_all[s, span, :] += value
            dk_all[s, span, :] += key
            dq_all[s, pl.ds(starts[i], QWIN), :] = gather_heads(query)
        for i, bias_part in enumerate(bias_parts):
            _, same = window_mask(codes, own_codes, g * GROUP + i)
            bias_acc[...] += jnp.where(same, bias_part, 0.0)
        return carry

    for g in range(windows // GROUP):
        backward_group(g, 0)

    rim = jnp.zeros((HALO, channels), BF16)

    def projection(c, gain_grad):
        parts = []
        for i in range(SPAN):
            s = c * SPAN + i
            back_q = jnp.concatenate([rim, (dq_all[s] * scale).astype(BF16), rim], axis=0)
            back_k = (dk_all[s] * scale).astype(BF16)
            parts.append(jnp.concatenate([back_q, back_k, dv_all[s].astype(BF16)], axis=1))
        back_all = jnp.concatenate(parts, axis=0)
        back_normed = mm_nt(back_all, project_weight[...])

        def with_rims(own, rims):
            pieces = []
            for i in range(SPAN):
                s = c * SPAN + i
                low = rims[s * HALO : (s + 1) * HALO, :]
                high = rims[halo_rows + s * HALO : halo_rows + (s + 1) * HALO, :]
                pieces += [low, own[s], high]
            return jnp.concatenate(pieces, axis=0)

        normed = with_rims(norm_own, norm_rim)
        unit = with_rims(unit_own, unit_rim)
        grad_project = mm_tn(normed, back_all)
        for i in range(3):
            project_grads[c, pl.ds(i * channels, channels), :] = grad_project[:, i * LANES : (i + 1) * LANES]
        gain_grad = gain_grad + column_sum(back_normed * unit)
        for i in range(SPAN):
            s = c * SPAN + i
            one = back_normed[i * ext : (i + 1) * ext]
            back_norm[s] = one[HALO : HALO + atoms]
            rows = pl.ds(pl.multiple_of(s * HALO, HALO), HALO)
            low = one[:HALO]
            high = one[HALO + atoms :]
            to_partner[rows, :] = jnp.where(is_odd, low, high).astype(BF16)
            to_link[rows, :] = jnp.where(is_odd, high, low).astype(BF16)
        return gain_grad

    gain_grad_one = zero_row
    for c in range(samples // SPAN):
        gain_grad_one = projection(c, gain_grad_one)

    tail = 8 * channels + TRANS
    lead = 3 * channels

    def add_up(parts, start, stop):
        total = parts[0, start:stop, :]
        for c in range(1, parts.shape[0]):
            total = total + parts[c, start:stop, :]
        return total

    slots = total_sums.shape[0] - tail - SLOT
    device = lax.axis_index("samp") * places + place
    total_sums[:lead, :] = add_up(project_grads, 0, lead)
    total_sums[lead:tail, :] = add_up(grads, lead, tail)
    total_sums[tail : tail + SLOT, :] = jnp.concatenate(
        [gain_grad_one, gain_grad_two, jnp.zeros((SLOT - 2, channels), F32)], axis=0
    )
    total_sums[tail + SLOT :, :] = bias_slots(column_sum(bias_acc[...]), device, slots)
    half = packed_keep.shape[0]
    mine = place % 2
    packed_keep[...] = total_sums[pl.ds(pl.multiple_of(mine * half, 8), half), :].astype(BF16)
    packed_send[...] = total_sums[pl.ds(pl.multiple_of((1 - mine) * half, 8), half), :].astype(BF16)


def lead_kernel(out):
    out[...] = jnp.zeros_like(out)


def pack_kernel(valid, blank, state, token, own_codes, partner, link, line):
    samples, atoms, _ = state.shape
    odd = lax.axis_index("atom") % 2
    for target, start in (
        (partner, (1 - odd) * (atoms - HALO)),
        (link, odd * (atoms - HALO)),
    ):
        for s in range(samples):
            target[s * HALO : (s + 1) * HALO, :] = state[s, pl.ds(pl.multiple_of(start, 16), HALO), :]
    rows = own_codes.shape[0]
    line[...] = jnp.zeros_like(line)
    line[:, :atoms] = token[...].reshape(1, atoms)
    lane = lax.broadcasted_iota(jnp.int32, (1, LANES), 1)
    codes = []
    for r in range(rows):
        limit = jnp.zeros((1, LANES), jnp.int32)
        for i in range(LANES // QWIN):
            w = r * (LANES // QWIN) + i
            if w * QWIN < atoms:
                limit = jnp.where(lane // QWIN == i, valid[w], limit)
        code = jnp.where(lane % QWIN < limit, line[:, r * LANES : (r + 1) * LANES] + 1, 0)
        codes.append(code)
        own_codes[r : r + 1, :] = code.astype(F32)
    tail_row = blank[0:14, :]
    ends = []
    for code in (codes[0], codes[-1]):
        ends.append(
            jnp.concatenate([(code // 256).astype(F32), (code % 256).astype(F32), tail_row], axis=0)
        )
    base = samples * HALO
    partner[base:, :] = jnp.where(odd == 1, ends[0], ends[1]).astype(BF16)
    link[base:, :] = jnp.where(odd == 1, ends[1], ends[0]).astype(BF16)


def rim_kernel(state, gain, back_norm, back_res, pair_back, link_back, out):
    samples, atoms, channels = state.shape
    is_odd = lax.axis_index("atom") % 2 == 1
    from_before = jnp.where(is_odd, pair_back[...], link_back[...]).astype(F32)
    from_after = jnp.where(is_odd, link_back[...], pair_back[...]).astype(F32)
    for s in range(samples):
        grad = back_norm[s]
        part = slice(s * HALO, (s + 1) * HALO)
        grad = jnp.concatenate(
            [
                grad[:HALO] + from_before[part],
                grad[HALO : atoms - HALO],
                grad[atoms - HALO :] + from_after[part],
            ],
            axis=0,
        )
        unit, inverse = split_norm(state[s].astype(F32))
        out[s] = (back_res[s] + norm_grad(grad * gain[0:1, :], unit, inverse)).astype(BF16)


def clip_kernel(own, other, attend, project, output, bias, transit_gain, transit, back):
    channels = LANES
    first = lax.axis_index("atom") % 2 == 0
    low = jnp.where(first, own[...], other[...]).astype(F32)
    high = jnp.where(first, other[...], own[...]).astype(F32)
    total = jnp.concatenate([low, high], axis=0)
    tail = 8 * channels + TRANS
    lane = lax.broadcasted_iota(jnp.int32, (1, LANES), 1)
    digits = column_sum(total[tail + SLOT :])
    heads = jnp.zeros((1, LANES), F32)
    for h in range(HEADS):
        sum_h = jnp.sum(jnp.where((lane // 4) % 4 == h, digits, 0.0), axis=1, keepdims=True)
        heads = jnp.where(lane == h, sum_h, heads)
    plain = total[: tail + SLOT]
    squares = jnp.sum(column_sum(plain * plain) + heads * heads, axis=1, keepdims=True)
    factor = CLIP_NORM * lax.rsqrt(squares + CLIP_NORM * CLIP_NORM)
    for i in range(3):
        project[:, i * LANES : (i + 1) * LANES] = total[i * channels : (i + 1) * channels] * factor
    output[...] = total[3 * channels : 4 * channels] * factor
    for i in range(2 * TRANS // LANES):
        transit[:, i * LANES : (i + 1) * LANES] = total[(4 + i) * channels : (5 + i) * channels] * factor
    back[...] = total[8 * channels : 8 * channels + TRANS] * factor
    attend[...] = total[tail : tail + 1] * factor
    transit_gain[...] = total[tail + 1 : tail + 2] * factor
    bias[...] = (heads * factor)[:, :HEADS]


def swap(value, axis, mask):
    return lax.ppermute(value, axis, [(i, i ^ mask) for i in range(lax.axis_size(axis))])


def pair_exchange(to_partner, to_link, axis):
    size = lax.axis_size(axis)
    links = [(i, (i + 1) % size) for i in range(1, size, 2)]
    links = links + [(j, i) for i, j in links]
    return lax.ppermute(to_link, axis, links), swap(to_partner, axis, 1)


VMEM = pl.BlockSpec(memory_space=pltpu.VMEM)
SMEM = pl.BlockSpec(memory_space=pltpu.SMEM)


def call(kernel, operands, specs, outs, scratch=(), flops=0, limit=16):
    moved = sum(x.size * x.dtype.itemsize for x in operands)
    return pl.pallas_call(
        kernel,
        out_shape=[jax.ShapeDtypeStruct(shape, dtype) for shape, dtype in outs],
        in_specs=list(specs),
        out_specs=[VMEM] * len(outs),
        scratch_shapes=list(scratch),
        cost_estimate=pl.CostEstimate(flops=flops, bytes_accessed=moved + flops // 200, transcendentals=0),
        compiler_params=pltpu.CompilerParams(vmem_limit_bytes=limit * 1024 * 1024),
    )(*operands)


def on_device(
    atom_state,
    atom_token,
    window_valid,
    attend_gain,
    project_weight,
    output_weight,
    token_bias,
    transit_gain,
    transit_weight,
    return_weight,
    cotangent,
):
    samples, atoms, channels = atom_state.shape
    ext = atoms + 2 * HALO
    windows = atoms // QWIN
    place = lax.axis_index("atom")
    devices = lax.axis_size("samp") * lax.axis_size("atom")
    slots = -(-devices * SLOT // LANES // SLOT) * SLOT
    total_rows = 8 * channels + TRANS + SLOT + slots
    half = total_rows // 2
    code_rows = -(-atoms // LANES)
    halo_rows = samples * HALO
    pack_rows = halo_rows + SLOT
    (blank,) = call(lead_kernel, (), (), (((SLOT, LANES), F32),), flops=10_000_000_000)
    own_codes, to_partner, to_link = call(
        pack_kernel,
        (window_valid, blank, atom_state, atom_token),
        (SMEM, VMEM, VMEM, VMEM),
        (
            ((code_rows, LANES), F32),
            ((pack_rows, channels), BF16),
            ((pack_rows, channels), BF16),
        ),
        (
            pltpu.VMEM((1, code_rows * LANES), jnp.int32),
        ),
        flops=10_000_000_000,
    )
    link_rows, pair_rows = pair_exchange(to_partner, to_link, "atom")
    vectors = jnp.stack([attend_gain, transit_gain, jnp.repeat(token_bias, QWIN)])
    rows_shape = (samples, atoms, channels)
    inner = call(
        inner_kernel,
        (own_codes, vectors, atom_state, project_weight),
        (VMEM,) * 4,
        (
            (rows_shape, BF16),
            (rows_shape, F32),
            (rows_shape, BF16),
            (rows_shape, BF16),
            (rows_shape, BF16),
            ((windows * samples, KWIN, HEADS * QWIN), F32),
            (rows_shape, BF16),
        ),
        (pltpu.VMEM((ext, LANES), F32),),
        flops=2_000_000_000,
    )
    block_out, back_norm, back_res, to_partner, to_link, keep, send = call(
        block_kernel,
        (
            own_codes,
            pair_rows,
            link_rows,
            vectors,
            *inner,
            atom_state,
            project_weight,
            output_weight,
            transit_weight,
            return_weight,
            cotangent,
        ),
        (VMEM,) * 17,
        (
            ((samples, atoms, channels), BF16),
            ((samples, atoms, channels), F32),
            ((samples, atoms, channels), F32),
            ((halo_rows, channels), BF16),
            ((halo_rows, channels), BF16),
            ((half, channels), BF16),
            ((half, channels), BF16),
        ),
        (
            pltpu.VMEM((2 * halo_rows, channels), BF16),
            pltpu.VMEM((2 * halo_rows, channels), F32),
            pltpu.VMEM((samples, ext, channels), BF16),
            pltpu.VMEM((samples, ext, channels), BF16),
            pltpu.VMEM((ext, LANES), F32),
            pltpu.VMEM((windows * samples, KWIN, HEADS * QWIN), F32),
            pltpu.VMEM((samples, atoms, channels), BF16),
            pltpu.VMEM((samples, atoms, channels), BF16),
            pltpu.VMEM((samples, atoms, channels), F32),
            pltpu.VMEM((samples, ext, channels), F32),
            pltpu.VMEM((samples, ext, channels), F32),
            pltpu.VMEM((samples // CHUNK, 8 * channels + TRANS, channels), F32),
            pltpu.VMEM((samples // SPAN, 3 * channels, channels), F32),
            pltpu.VMEM((total_rows, channels), F32),
            pltpu.VMEM((KWIN, HEADS * QWIN), F32),
        ),
        flops=4_000_000_000,
        limit=24,
    )

    link_back, pair_back = pair_exchange(to_partner, to_link, "atom")
    cores = lax.axis_size("atom")
    part = keep + swap(send, "atom", 1)
    x_bit = (place // 2) % 2
    quarter = half // 2
    mine = lax.dynamic_slice_in_dim(part, x_bit * quarter, quarter)
    theirs = lax.dynamic_slice_in_dim(part, (1 - x_bit) * quarter, quarter)
    sums = mine + swap(theirs, "atom", 2)
    mask = 4
    while mask < cores:
        sums = sums + swap(sums, "atom", mask)
        mask *= 2
    sums, link_back, pair_back = lax.optimization_barrier((sums, link_back, pair_back))
    (state_grad,) = call(
        rim_kernel,
        (atom_state, vectors, back_norm, back_res, pair_back, link_back),
        (VMEM,) * 6,
        (((samples, atoms, channels), BF16),),
        flops=100_000_000,
    )
    mask = 1
    while mask < lax.axis_size("samp"):
        sums = sums + swap(sums, "samp", mask)
        mask *= 2
    sums, state_grad = lax.optimization_barrier((sums, state_grad))
    other = swap(sums, "atom", 2)
    sums = jnp.where(
        x_bit == 0,
        jnp.concatenate([sums, other], axis=0),
        jnp.concatenate([other, sums], axis=0),
    )
    other = swap(sums, "atom", 1)
    clipped = call(
        clip_kernel,
        (sums, other),
        (VMEM,) * 2,
        (
            ((1, channels), F32),
            ((channels, 3 * channels), F32),
            ((channels, channels), F32),
            ((1, HEADS), F32),
            ((1, channels), F32),
            ((channels, 2 * TRANS), F32),
            ((TRANS, channels), F32),
        ),
    )
    return (
        block_out,
        state_grad,
        clipped[0].reshape(channels),
        clipped[1],
        clipped[2],
        clipped[3].reshape(HEADS),
        clipped[4].reshape(channels),
        clipped[5],
        clipped[6],
    )


def solution(mesh):
    return jax.shard_map(
        on_device,
        mesh=mesh,
        in_specs=(
            P("samp", "atom", None),
            P("atom"),
            P("atom"),
            P(),
            P(),
            P(),
            P(),
            P(),
            P(),
            P(),
            P("samp", "atom", None),
        ),
        out_specs=(
            P("samp", "atom", None),
            P("samp", "atom", None),
            P(),
            P(),
            P(),
            P(),
            P(),
            P(),
            P(),
        ),
        check_vma=False,
    )
```

```python
import functools
import math

import jax
import jax.numpy as jnp
from jax import lax
from jax.experimental import pallas as pl
from jax.experimental.pallas import tpu as pltpu
from jax.sharding import PartitionSpec as P

HEADS = 4
TRANS = 256
QWIN = 32
KWIN = 128
HALO = 48
EPSILON = 1e-05
CLIP_NORM = 256.0
LANES = 128
GROUP = 10
CHUNK = 4
SPAN = 4
SLOT = 16
LOG2E = 1.0 / math.log(2.0)

F32 = jnp.float32
BF16 = jnp.bfloat16


def mm(a, b):
    return lax.dot_general(a, b, (((1,), (0,)), ((), ())), preferred_element_type=F32)


def mm_nt(a, b):
    return lax.dot_general(a, b, (((1,), (1,)), ((), ())), preferred_element_type=F32)


def mm_tn(a, b):
    return lax.dot_general(a, b, (((0,), (0,)), ((), ())), preferred_element_type=F32)


def row_mean(x):
    return jnp.sum(x, axis=-1, keepdims=True) * (1.0 / x.shape[-1])


def column_sum(x):
    return jnp.sum(x, axis=0, keepdims=True)


def split_norm(x):
    shifted = x - row_mean(x)
    inverse = lax.rsqrt(row_mean(shifted * shifted) + EPSILON)
    return shifted * inverse, inverse


def norm_grad(grad, unit, inverse):
    return inverse * (grad - row_mean(grad) - unit * row_mean(grad * unit))


def head_of_lane(rows):
    return lax.broadcasted_iota(jnp.int32, (rows, LANES), 1) // (LANES // HEADS)


def spread_heads(rows):
    head = head_of_lane(QWIN)
    return jnp.concatenate(
        [jnp.where(head == h, rows, jnp.zeros_like(rows)) for h in range(HEADS)], axis=0
    )


def gather_heads(rows):
    head = head_of_lane(QWIN)
    total = rows[:QWIN]
    for h in range(1, HEADS):
        total = jnp.where(head == h, rows[h * QWIN : (h + 1) * QWIN], total)
    return total


def bias_slots(row, place, rows):
    slot_lane = lax.broadcasted_iota(jnp.int32, (1, LANES), 1)
    width = LANES // HEADS
    line = jnp.zeros((1, LANES), F32)
    for h in range(HEADS):
        inside = (slot_lane // width) == h
        total = jnp.sum(jnp.where(inside, row, 0.0), axis=1, keepdims=True)
        high = total.astype(BF16).astype(F32)
        middle = (total - high).astype(BF16).astype(F32)
        low = total - high - middle
        for digit, value in enumerate((high, middle, low)):
            line = jnp.where(slot_lane % SLOT == h * 4 + digit, value, line)
    per_row = LANES // SLOT
    lane = lax.broadcasted_iota(jnp.int32, (rows, LANES), 1)
    row_index = lax.broadcasted_iota(jnp.int32, (rows, LANES), 0)
    here = (lane // SLOT == place % per_row) & (row_index == place // per_row)
    return jnp.where(here, jnp.broadcast_to(line, (rows, LANES)), 0.0)


def is_inner(w, atoms):
    return w * QWIN >= HALO and w * QWIN + KWIN - HALO <= atoms


def down_lanes(row):
    return jnp.transpose(jnp.broadcast_to(row, (LANES, LANES)))


def fill_own_codes(codes, own_codes, atoms):
    for i in range(own_codes.shape[0]):
        count = min(LANES, atoms - i * LANES)
        start = HALO + i * LANES
        codes[start : start + count, :] = down_lanes(own_codes[i : i + 1, :])[0:count]


def query_row(own_codes, w):
    row, lane = divmod(w * QWIN, LANES)
    return jnp.concatenate([own_codes[row : row + 1, lane : lane + QWIN]] * HEADS, axis=1)


def window_mask(codes, own_codes, w):
    key_code = codes[w * QWIN : w * QWIN + KWIN, :]
    return key_code, key_code == query_row(own_codes, w)


def attend_windows(picked, samples, query_of, key_of, value_of, codes, own_codes, bias_row, probs, att):
    scale = 1.0 / math.sqrt(LANES // HEADS)
    units = [(w, s) for w in picked for s in range(samples)]
    scores = [mm_nt(key_of(s, w), spread_heads(query_of(s, w))) for w, s in units]
    offsets = {}
    for w in picked:
        key_code, same = window_mask(codes, own_codes, w)
        offset = jnp.where(same, bias_row * LOG2E, 0.0)
        offsets[w] = jnp.where(key_code > 0, offset, -1e30)
    packed = []
    for (w, s), score in zip(units, scores):
        score = score * (scale * LOG2E) + offsets[w]
        weights = jnp.exp2(score - jnp.max(score, axis=0, keepdims=True))
        weights = weights * (1.0 / column_sum(weights))
        probs[w * samples + s] = weights
        packed.append(weights.astype(BF16))
    outcomes = [mm_tn(weights, value_of(s, w)) for (w, s), weights in zip(units, packed)]
    for (w, s), outcome in zip(units, outcomes):
        att[s, w * QWIN : (w + 1) * QWIN, :] = gather_heads(outcome).astype(BF16)


def inner_kernel(
    own_codes, vectors, state, project_weight, norm_own, unit_own, q_own, k_own, v_own, probs, att, codes
):
    samples, atoms, channels = state.shape
    fill_own_codes(codes, own_codes, atoms)
    for s in range(samples):
        unit, _ = split_norm(state[s].astype(F32))
        unit_own[s] = unit
        normed = (unit * vectors[0:1, :]).astype(BF16)
        norm_own[s] = normed
        projected = mm(normed, project_weight[...]).astype(BF16)
        q_own[s] = projected[:, :channels]
        k_own[s] = projected[:, channels : 2 * channels]
        v_own[s] = projected[:, 2 * channels :]

    def own_window(ref, s, w):
        return ref[s, w * QWIN - HALO : w * QWIN - HALO + KWIN, :]

    attend_windows(
        [w for w in range(atoms // QWIN) if is_inner(w, atoms)],
        samples,
        lambda s, w: q_own[s, w * QWIN : (w + 1) * QWIN, :],
        lambda s, w: own_window(k_own, s, w),
        lambda s, w: own_window(v_own, s, w),
        codes,
        own_codes,
        vectors[2:3, :],
        probs,
        att,
    )


def block_kernel(
    own_codes,
    pair_rows,
    link_rows,
    vectors,
    norm_own,
    unit_own,
    q_all,
    k_own,
    v_own,
    probs_own,
    att_own,
    state,
    project_weight,
    output_weight,
    transit_weight,
    return_weight,
    cot,
    block_out,
    back_norm,
    back_res,
    to_partner,
    to_link,
    packed_keep,
    packed_send,
    norm_rim,
    unit_rim,
    k_all,
    v_all,
    codes,
    probs,
    att,
    d_att,
    dq_all,
    dk_all,
    dv_all,
    grads,
    project_grads,
    total_sums,
    bias_acc,
):
    samples, atoms, channels = state.shape
    ext = atoms + 2 * HALO
    windows = atoms // QWIN
    place = lax.axis_index("atom")
    places = lax.axis_size("atom")
    is_odd = place % 2 == 1
    halo_rows = samples * HALO
    scale = 1.0 / math.sqrt(channels // HEADS)
    before = jnp.where(is_odd, pair_rows[...], link_rows[...])
    after = jnp.where(is_odd, link_rows[...], pair_rows[...])

    def edge_codes(part):
        high = part[halo_rows : halo_rows + 1, :].astype(F32)
        low = part[halo_rows + 1 : halo_rows + 2, :].astype(F32)
        return high * 256.0 + low

    first_code = jnp.where(place == 0, 0.0, edge_codes(before))
    last_code = jnp.where(place == places - 1, 0.0, edge_codes(after))
    last_lane = (atoms - HALO) % LANES
    codes[0:HALO, :] = down_lanes(first_code)[last_lane : last_lane + HALO]
    fill_own_codes(codes, own_codes, atoms)
    codes[HALO + atoms : ext, :] = down_lanes(last_code)[0:HALO]

    bias_acc[...] = jnp.zeros_like(bias_acc)
    dk_all[...] = jnp.zeros_like(dk_all)
    dv_all[...] = jnp.zeros_like(dv_all)

    gain_one = vectors[0:1, :]
    gain_two = vectors[1:2, :]
    bias_row = vectors[2:3, :]
    keep_rows = KWIN - QWIN + HALO
    keep_rows = min(atoms, keep_rows + QWIN)
    both_rims = jnp.concatenate([before[:halo_rows], after[:halo_rows]], axis=0).astype(F32)
    unit, _ = split_norm(both_rims)
    unit_rim[...] = unit
    normed = (unit * gain_one).astype(BF16)
    norm_rim[...] = normed
    rim_pairs = mm(normed, project_weight[:, channels:]).astype(BF16)
    for ref, own, column in ((k_all, k_own, 0), (v_all, v_own, channels)):
        part = rim_pairs[:, column : column + channels]
        for s in range(samples):
            ref[s, :HALO, :] = part[s * HALO : (s + 1) * HALO]
            ref[s, HALO : HALO + keep_rows, :] = own[s, :keep_rows, :]
            ref[s, HALO + atoms - keep_rows : HALO + atoms, :] = own[s, atoms - keep_rows :, :]
            ref[s, HALO + atoms :, :] = part[halo_rows + s * HALO : halo_rows + (s + 1) * HALO]

    def pair_window(ext_ref, own_ref, s, w):
        if is_inner(w, atoms):
            return own_ref[s, w * QWIN - HALO : w * QWIN - HALO + KWIN, :]
        return ext_ref[s, w * QWIN : w * QWIN + KWIN, :]

    def key_of(s, w):
        return pair_window(k_all, k_own, s, w)

    def value_of(s, w):
        return pair_window(v_all, v_own, s, w)

    def query_of(s, w):
        return q_all[s, w * QWIN : (w + 1) * QWIN, :]

    def prob_of(s, w):
        return (probs_own if is_inner(w, atoms) else probs)[w * samples + s]

    outer = [w for w in range(windows) if not is_inner(w, atoms)]
    attend_windows(
        outer, samples, query_of, key_of, value_of, codes, own_codes, bias_row, probs, att
    )
    for s in range(samples):
        for w in range(windows):
            if is_inner(w, atoms):
                span = slice(w * QWIN, (w + 1) * QWIN)
                att[s, span, :] = att_own[s, span, :]

    def group_units(g):
        starts = [(g * GROUP + i) * QWIN for i in range(GROUP)]
        return starts, [(i, s) for i in range(GROUP) for s in range(samples)]

    chunk_rows = CHUNK * atoms

    def flat(ref, c):
        return ref[pl.ds(c * CHUNK, CHUNK)].reshape(chunk_rows, channels)

    def fill(ref, c, value):
        ref[pl.ds(c * CHUNK, CHUNK)] = value.reshape(CHUNK, atoms, channels)

    def transition(c, gain_grad):
        attended = flat(att, c)
        residual = (flat(state, c).astype(F32) + mm(attended, output_weight[...])).astype(BF16)
        residual = residual.astype(F32)
        unit, inverse = split_norm(residual)
        transit_in = (unit * gain_two).astype(BF16)
        both = mm(transit_in, transit_weight[...])
        gate = both[:, :TRANS]
        up = both[:, TRANS:]
        sigmoid = 1.0 / (1.0 + jnp.exp2(gate * -LOG2E))
        silu = gate * sigmoid
        gated = (silu * up).astype(BF16)
        fill(block_out, c, (residual + mm(gated, return_weight[...])).astype(BF16))
        cot16 = flat(cot, c)
        back_gated = mm_nt(cot16, return_weight[...])
        back_gate = back_gated * up * (sigmoid + silu * (1.0 - sigmoid))
        back_hidden = jnp.concatenate([back_gate, back_gated * silu], axis=1).astype(BF16)
        grads[c, pl.ds(8 * channels, TRANS), :] = mm_tn(gated, cot16)
        grad_transit = mm_tn(transit_in, back_hidden)
        for i in range(2 * TRANS // LANES):
            grads[c, pl.ds((4 + i) * channels, channels), :] = grad_transit[:, i * LANES : (i + 1) * LANES]
        back_transit = mm_nt(back_hidden, transit_weight[...])
        gain_grad = gain_grad + column_sum(back_transit * unit)
        back_residual = cot16.astype(F32) + norm_grad(back_transit * gain_two, unit, inverse)
        fill(back_res, c, back_residual)
        back16 = back_residual.astype(BF16)
        grads[c, pl.ds(3 * channels, channels), :] = mm_tn(attended, back16)
        fill(d_att, c, mm_nt(back16, output_weight[...]).astype(BF16))
        return gain_grad

    zero_row = jnp.zeros((1, channels), F32)
    gain_grad_two = zero_row
    for c in range(samples // CHUNK):
        gain_grad_two = transition(c, gain_grad_two)

    def backward_group(g, carry):
        starts, units = group_units(g)
        backs = [spread_heads(d_att[s, pl.ds(starts[i], QWIN), :]) for i, s in units]
        back_weights = [
            mm_nt(value_of(s, g * GROUP + i), back) for (i, s), back in zip(units, backs)
        ]
        packed = []
        scores16 = []
        bias_parts = [None] * GROUP
        for (i, s), back_weight in zip(units, back_weights):
            weights = prob_of(s, g * GROUP + i)
            weighted = weights * back_weight
            back_scores = weighted - weights * column_sum(weighted)
            bias_parts[i] = back_scores if bias_parts[i] is None else bias_parts[i] + back_scores
            packed.append(weights.astype(BF16))
            scores16.append(back_scores.astype(BF16))
        back_values = [mm(weights, back) for weights, back in zip(packed, backs)]
        back_keys = [
            mm(scores, spread_heads(q_all[s, pl.ds(starts[i], QWIN), :]))
            for (i, s), scores in zip(units, scores16)
        ]
        back_queries = [
            mm_tn(scores, key_of(s, g * GROUP + i))
            for (i, s), scores in zip(units, scores16)
        ]
        for (i, s), value, key, query in zip(units, back_values, back_keys, back_queries):
            span = pl.ds(starts[i], KWIN)
            dv_all[s, span, :] += value
            dk_all[s, span, :] += key
            dq_all[s, pl.ds(starts[i], QWIN), :] = gather_heads(query)
        for i, bias_part in enumerate(bias_parts):
            _, same = window_mask(codes, own_codes, g * GROUP + i)
            bias_acc[...] += jnp.where(same, bias_part, 0.0)
        return carry

    for g in range(windows // GROUP):
        backward_group(g, 0)

    rim = jnp.zeros((HALO, channels), BF16)

    def projection(c, gain_grad):
        parts = []
        for i in range(SPAN):
            s = c * SPAN + i
            back_q = jnp.concatenate([rim, (dq_all[s] * scale).astype(BF16), rim], axis=0)
            back_k = (dk_all[s] * scale).astype(BF16)
            parts.append(jnp.concatenate([back_q, back_k, dv_all[s].astype(BF16)], axis=1))
        back_all = jnp.concatenate(parts, axis=0)
        back_normed = mm_nt(back_all, project_weight[...])

        def with_rims(own, rims):
            pieces = []
            for i in range(SPAN):
                s = c * SPAN + i
                low = rims[s * HALO : (s + 1) * HALO, :]
                high = rims[halo_rows + s * HALO : halo_rows + (s + 1) * HALO, :]
                pieces += [low, own[s], high]
            return jnp.concatenate(pieces, axis=0)

        normed = with_rims(norm_own, norm_rim)
        unit = with_rims(unit_own, unit_rim)
        grad_project = mm_tn(normed, back_all)
        for i in range(3):
            project_grads[c, pl.ds(i * channels, channels), :] = grad_project[:, i * LANES : (i + 1) * LANES]
        gain_grad = gain_grad + column_sum(back_normed * unit)
        for i in range(SPAN):
            s = c * SPAN + i
            one = back_normed[i * ext : (i + 1) * ext]
            back_norm[s] = one[HALO : HALO + atoms]
            rows = pl.ds(pl.multiple_of(s * HALO, HALO), HALO)
            low = one[:HALO]
            high = one[HALO + atoms :]
            to_partner[rows, :] = jnp.where(is_odd, low, high).astype(BF16)
            to_link[rows, :] = jnp.where(is_odd, high, low).astype(BF16)
        return gain_grad

    gain_grad_one = zero_row
    for c in range(samples // SPAN):
        gain_grad_one = projection(c, gain_grad_one)

    tail = 8 * channels + TRANS
    lead = 3 * channels

    def add_up(parts, start, stop):
        total = parts[0, start:stop, :]
        for c in range(1, parts.shape[0]):
            total = total + parts[c, start:stop, :]
        return total

    slots = total_sums.shape[0] - tail - SLOT
    device = lax.axis_index("samp") * places + place
    total_sums[:lead, :] = add_up(project_grads, 0, lead)
    total_sums[lead:tail, :] = add_up(grads, lead, tail)
    total_sums[tail : tail + SLOT, :] = jnp.concatenate(
        [gain_grad_one, gain_grad_two, jnp.zeros((SLOT - 2, channels), F32)], axis=0
    )
    total_sums[tail + SLOT :, :] = bias_slots(column_sum(bias_acc[...]), device, slots)
    half = packed_keep.shape[0]
    mine = place % 2
    packed_keep[...] = total_sums[pl.ds(pl.multiple_of(mine * half, 8), half), :].astype(BF16)
    packed_send[...] = total_sums[pl.ds(pl.multiple_of((1 - mine) * half, 8), half), :].astype(BF16)


def lead_kernel(out):
    out[...] = jnp.zeros_like(out)


def pack_kernel(valid, blank, state, token, own_codes, partner, link, line):
    samples, atoms, _ = state.shape
    odd = lax.axis_index("atom") % 2
    for target, start in (
        (partner, (1 - odd) * (atoms - HALO)),
        (link, odd * (atoms - HALO)),
    ):
        for s in range(samples):
            target[s * HALO : (s + 1) * HALO, :] = state[s, pl.ds(pl.multiple_of(start, 16), HALO), :]
    rows = own_codes.shape[0]
    line[...] = jnp.zeros_like(line)
    line[:, :atoms] = token[...].reshape(1, atoms)
    lane = lax.broadcasted_iota(jnp.int32, (1, LANES), 1)
    codes = []
    for r in range(rows):
        limit = jnp.zeros((1, LANES), jnp.int32)
        for i in range(LANES // QWIN):
            w = r * (LANES // QWIN) + i
            if w * QWIN < atoms:
                limit = jnp.where(lane // QWIN == i, valid[w], limit)
        code = jnp.where(lane % QWIN < limit, line[:, r * LANES : (r + 1) * LANES] + 1, 0)
        codes.append(code)
        own_codes[r : r + 1, :] = code.astype(F32)
    tail_row = blank[0:14, :]
    ends = []
    for code in (codes[0], codes[-1]):
        ends.append(
            jnp.concatenate([(code // 256).astype(F32), (code % 256).astype(F32), tail_row], axis=0)
        )
    base = samples * HALO
    partner[base:, :] = jnp.where(odd == 1, ends[0], ends[1]).astype(BF16)
    link[base:, :] = jnp.where(odd == 1, ends[1], ends[0]).astype(BF16)


def rim_kernel(state, gain, back_norm, back_res, pair_back, link_back, out):
    samples, atoms, channels = state.shape
    is_odd = lax.axis_index("atom") % 2 == 1
    from_before = jnp.where(is_odd, pair_back[...], link_back[...]).astype(F32)
    from_after = jnp.where(is_odd, link_back[...], pair_back[...]).astype(F32)
    for s in range(samples):
        grad = back_norm[s]
        part = slice(s * HALO, (s + 1) * HALO)
        grad = jnp.concatenate(
            [
                grad[:HALO] + from_before[part],
                grad[HALO : atoms - HALO],
                grad[atoms - HALO :] + from_after[part],
            ],
            axis=0,
        )
        unit, inverse = split_norm(state[s].astype(F32))
        out[s] = (back_res[s] + norm_grad(grad * gain[0:1, :], unit, inverse)).astype(BF16)


def clip_kernel(own, other, attend, project, output, bias, transit_gain, transit, back):
    channels = LANES
    first = lax.axis_index("atom") % 2 == 0
    low = jnp.where(first, own[...], other[...]).astype(F32)
    high = jnp.where(first, other[...], own[...]).astype(F32)
    total = jnp.concatenate([low, high], axis=0)
    tail = 8 * channels + TRANS
    lane = lax.broadcasted_iota(jnp.int32, (1, LANES), 1)
    digits = column_sum(total[tail + SLOT :])
    heads = jnp.zeros((1, LANES), F32)
    for h in range(HEADS):
        sum_h = jnp.sum(jnp.where((lane // 4) % 4 == h, digits, 0.0), axis=1, keepdims=True)
        heads = jnp.where(lane == h, sum_h, heads)
    plain = total[: tail + SLOT]
    squares = jnp.sum(column_sum(plain * plain) + heads * heads, axis=1, keepdims=True)
    factor = CLIP_NORM * lax.rsqrt(squares + CLIP_NORM * CLIP_NORM)
    for i in range(3):
        project[:, i * LANES : (i + 1) * LANES] = total[i * channels : (i + 1) * channels] * factor
    output[...] = total[3 * channels : 4 * channels] * factor
    for i in range(2 * TRANS // LANES):
        transit[:, i * LANES : (i + 1) * LANES] = total[(4 + i) * channels : (5 + i) * channels] * factor
    back[...] = total[8 * channels : 8 * channels + TRANS] * factor
    attend[...] = total[tail : tail + 1] * factor
    transit_gain[...] = total[tail + 1 : tail + 2] * factor
    bias[...] = (heads * factor)[:, :HEADS]


def swap(value, axis, mask):
    return lax.ppermute(value, axis, [(i, i ^ mask) for i in range(lax.axis_size(axis))])


def pair_exchange(to_partner, to_link, axis):
    size = lax.axis_size(axis)
    links = [(i, (i + 1) % size) for i in range(1, size, 2)]
    links = links + [(j, i) for i, j in links]
    return lax.ppermute(to_link, axis, links), swap(to_partner, axis, 1)


VMEM = pl.BlockSpec(memory_space=pltpu.VMEM)
SMEM = pl.BlockSpec(memory_space=pltpu.SMEM)


def call(kernel, operands, specs, outs, scratch=(), flops=0, limit=16):
    moved = sum(x.size * x.dtype.itemsize for x in operands)
    return pl.pallas_call(
        kernel,
        out_shape=[jax.ShapeDtypeStruct(shape, dtype) for shape, dtype in outs],
        in_specs=list(specs),
        out_specs=[VMEM] * len(outs),
        scratch_shapes=list(scratch),
        cost_estimate=pl.CostEstimate(flops=flops, bytes_accessed=moved + flops // 200, transcendentals=0),
        compiler_params=pltpu.CompilerParams(vmem_limit_bytes=limit * 1024 * 1024),
    )(*operands)


def on_device(
    atom_state,
    atom_token,
    window_valid,
    attend_gain,
    project_weight,
    output_weight,
    token_bias,
    transit_gain,
    transit_weight,
    return_weight,
    cotangent,
):
    samples, atoms, channels = atom_state.shape
    ext = atoms + 2 * HALO
    windows = atoms // QWIN
    place = lax.axis_index("atom")
    devices = lax.axis_size("samp") * lax.axis_size("atom")
    slots = -(-devices * SLOT // LANES // SLOT) * SLOT
    total_rows = 8 * channels + TRANS + SLOT + slots
    half = total_rows // 2
    code_rows = -(-atoms // LANES)
    halo_rows = samples * HALO
    pack_rows = halo_rows + SLOT
    (blank,) = call(lead_kernel, (), (), (((SLOT, LANES), F32),), flops=10_000_000_000)
    own_codes, to_partner, to_link = call(
        pack_kernel,
        (window_valid, blank, atom_state, atom_token),
        (SMEM, VMEM, VMEM, VMEM),
        (
            ((code_rows, LANES), F32),
            ((pack_rows, channels), BF16),
            ((pack_rows, channels), BF16),
        ),
        (
            pltpu.VMEM((1, code_rows * LANES), jnp.int32),
        ),
        flops=10_000_000_000,
    )
    link_rows, pair_rows = pair_exchange(to_partner, to_link, "atom")
    vectors = jnp.stack([attend_gain, transit_gain, jnp.repeat(token_bias, QWIN)])
    rows_shape = (samples, atoms, channels)
    inner = call(
        inner_kernel,
        (own_codes, vectors, atom_state, project_weight),
        (VMEM,) * 4,
        (
            (rows_shape, BF16),
            (rows_shape, F32),
            (rows_shape, BF16),
            (rows_shape, BF16),
            (rows_shape, BF16),
            ((windows * samples, KWIN, HEADS * QWIN), F32),
            (rows_shape, BF16),
        ),
        (pltpu.VMEM((ext, LANES), F32),),
        flops=2_000_000_000,
    )
    block_out, back_norm, back_res, to_partner, to_link, keep, send = call(
        block_kernel,
        (
            own_codes,
            pair_rows,
            link_rows,
            vectors,
            *inner,
            atom_state,
            project_weight,
            output_weight,
            transit_weight,
            return_weight,
            cotangent,
        ),
        (VMEM,) * 17,
        (
            ((samples, atoms, channels), BF16),
            ((samples, atoms, channels), F32),
            ((samples, atoms, channels), F32),
            ((halo_rows, channels), BF16),
            ((halo_rows, channels), BF16),
            ((half, channels), BF16),
            ((half, channels), BF16),
        ),
        (
            pltpu.VMEM((2 * halo_rows, channels), BF16),
            pltpu.VMEM((2 * halo_rows, channels), F32),
            pltpu.VMEM((samples, ext, channels), BF16),
            pltpu.VMEM((samples, ext, channels), BF16),
            pltpu.VMEM((ext, LANES), F32),
            pltpu.VMEM((windows * samples, KWIN, HEADS * QWIN), F32),
            pltpu.VMEM((samples, atoms, channels), BF16),
            pltpu.VMEM((samples, atoms, channels), BF16),
            pltpu.VMEM((samples, atoms, channels), F32),
            pltpu.VMEM((samples, ext, channels), F32),
            pltpu.VMEM((samples, ext, channels), F32),
            pltpu.VMEM((samples // CHUNK, 8 * channels + TRANS, channels), F32),
            pltpu.VMEM((samples // SPAN, 3 * channels, channels), F32),
            pltpu.VMEM((total_rows, channels), F32),
            pltpu.VMEM((KWIN, HEADS * QWIN), F32),
        ),
        flops=4_000_000_000,
        limit=24,
    )

    link_back, pair_back = pair_exchange(to_partner, to_link, "atom")
    cores = lax.axis_size("atom")
    part = keep + swap(send, "atom", 1)
    x_bit = (place // 2) % 2
    quarter = half // 2
    mine = lax.dynamic_slice_in_dim(part, x_bit * quarter, quarter)
    theirs = lax.dynamic_slice_in_dim(part, (1 - x_bit) * quarter, quarter)
    sums = mine + swap(theirs, "atom", 2)
    mask = 4
    while mask < cores:
        sums = sums + swap(sums, "atom", mask)
        mask *= 2
    sums, link_back, pair_back = lax.optimization_barrier((sums, link_back, pair_back))
    (state_grad,) = call(
        rim_kernel,
        (atom_state, vectors, back_norm, back_res, pair_back, link_back),
        (VMEM,) * 6,
        (((samples, atoms, channels), BF16),),
        flops=100_000_000,
    )
    mask = 1
    while mask < lax.axis_size("samp"):
        sums = sums + swap(sums, "samp", mask)
        mask *= 2
    sums, state_grad = lax.optimization_barrier((sums, state_grad))
    other = swap(sums, "atom", 2)
    sums = jnp.where(
        x_bit == 0,
        jnp.concatenate([sums, other], axis=0),
        jnp.concatenate([other, sums], axis=0),
    )
    other = swap(sums, "atom", 1)
    clipped = call(
        clip_kernel,
        (sums, other),
        (VMEM,) * 2,
        (
            ((1, channels), F32),
            ((channels, 3 * channels), F32),
            ((channels, channels), F32),
            ((1, HEADS), F32),
            ((1, channels), F32),
            ((channels, 2 * TRANS), F32),
            ((TRANS, channels), F32),
        ),
    )
    return (
        block_out,
        state_grad,
        clipped[0].reshape(channels),
        clipped[1],
        clipped[2],
        clipped[3].reshape(HEADS),
        clipped[4].reshape(channels),
        clipped[5],
        clipped[6],
    )


def solution(mesh):
    return jax.shard_map(
        on_device,
        mesh=mesh,
        in_specs=(
            P("samp", "atom", None),
            P("atom"),
            P("atom"),
            P(),
            P(),
            P(),
            P(),
            P(),
            P(),
            P(),
            P("samp", "atom", None),
        ),
        out_specs=(
            P("samp", "atom", None),
            P("samp", "atom", None),
            P(),
            P(),
            P(),
            P(),
            P(),
            P(),
            P(),
        ),
        check_vma=False,
    )
```
